128 devices in a mesh: dp: 1, cols: 64 (over z, y, x), rows: 2 (over core).
Axes of the slice: x: 4, y: 4, z: 4, core: 2. Of those that a mesh axis runs over, the one named last changes fastest.
Arguments:
- h_init: bfloat16 [1, 48, 4096, 192], P('dp', 'rows', 'cols')
- c_init: float32 [1, 48, 4096, 192], P('dp', 'rows', 'cols')
- w_rec: bfloat16 [3, 3, 192, 768], replicated
- gate_bias: float32 [16, 768], replicated
Outputs:
- output 1: bfloat16 [16, 1, 48, 4096, 192], P(None, 'dp', 'rows', 'cols')
- output 2: float32 [1, 48, 4096, 192], P('dp', 'rows', 'cols')
All inputs are finite; a program needn't handle non-finite values.
Results may differ from the reference program's by a relative error of at most 0.00320178.
Values are sent between devices in bfloat16 or wider.
A program may use at most 1 GiB of HBM per device.

```python
import jax
import jax.numpy as jnp
from jax import lax

STEPS = 16
BATCH = 1
GRID_H = 48
GRID_W = 4096
CHANNELS = 192


def setup_inputs(seed: int = 0, part: int = 0) -> dict:
    key_w, key_b = jax.random.split(jax.random.key(seed))
    part_key = jax.random.fold_in(jax.random.key(seed + 1), part)
    key_h, key_c = jax.random.split(part_key)
    fan_in = 9 * CHANNELS
    w_rec = (jax.random.normal(key_w, (3, 3, CHANNELS, 4 * CHANNELS), jnp.float32) * (1.5 * fan_in ** -0.5)).astype(jnp.bfloat16)
    gate_offset = jnp.repeat(jnp.array([0.0, 1.0, 0.0, 0.0], jnp.float32), CHANNELS)
    gate_bias = jax.random.normal(key_b, (STEPS, 4 * CHANNELS), jnp.float32) * 0.5 + gate_offset
    h_init = (jax.random.normal(key_h, (BATCH, GRID_H, GRID_W, CHANNELS), jnp.float32) * 0.6).astype(jnp.bfloat16)
    c_init = jax.random.normal(key_c, (BATCH, GRID_H, GRID_W, CHANNELS), jnp.float32)
    return {"h_init": h_init, "c_init": c_init, "w_rec": w_rec, "gate_bias": gate_bias}


def reference(h_init, c_init, w_rec, gate_bias):
    w_wide = w_rec.astype(jnp.float32)

    def one_step(carry_in, bias_row):
        h_prev, c_prev = carry_in
        gate_pre = lax.conv_general_dilated(h_prev.astype(jnp.float32), w_wide, (1, 1), "SAME", dimension_numbers=("NHWC", "HWIO", "NHWC")) + bias_row
        in_gate, forget_gate, out_gate, cand_gate = jnp.split(gate_pre, 4, axis=-1)
        c_next = jax.nn.sigmoid(forget_gate) * c_prev + jax.nn.sigmoid(in_gate) * jnp.tanh(cand_gate)
        h_next = (jax.nn.sigmoid(out_gate) * jnp.tanh(c_next)).astype(jnp.bfloat16)
        return (h_next, c_next), h_next

    final_state, h_seq = lax.scan(one_step, (h_init, c_init), gate_bias)
    return h_seq, final_state[1]
```

```python
import functools

import jax
import jax.numpy as jnp
from jax import lax
from jax.experimental import pallas as pl
from jax.experimental.pallas import tpu as pltpu
from jax.sharding import PartitionSpec as P

MESH = pl.DeviceIdType.MESH
F32 = jnp.float32
BF16 = jnp.bfloat16

STEPS = 16
ROWS = 24
COLS = 64
CH = 192
LANES = 128
HALF = 64
EDGE = 8
INNER = 48
PITCH = 80
GROWS = ROWS + 3
GATES = 4 * CH
DEPTH = 14 * LANES
WIDTH = 5 * LANES
EXT = 2 * ROWS
STRIP = 32

I_ROWS = [range(6 * j, 6 * j + 6) for j in range(4)]
E_ROWS = [range(9), range(9, ROWS)]


def lanes(n, count=1):
    return slice(LANES * n, LANES * (n + count))


def sigmoid(x):
    return 0.5 * jnp.tanh(0.5 * x) + 0.5


def at_row(r):
    return r * PITCH + EDGE


def kernel(h_init, c_init, w_hbm, bias_ref, h_seq, c_last, w_ref, ws_ref, fa0, fb0, fa1, fb1, hb0, hb1, ca, cb, sb, el, er,
           out0, out1, cio, bp, to_right, to_left, from_left, from_right, diag_left, diag_right, seam,
           w_sems, in_sems, out_sems, col_send, left_recv, right_recv, dleft_recv, dright_recv, seam_send, seam_recv):
    col_count = lax.axis_size("cols")
    core = lax.axis_index("rows")
    col = lax.axis_index("cols")
    other = 1 - core
    has_left = col > 0
    has_right = col < col_count - 1

    def out_row(y):
        return jnp.where(core == 0, y, ROWS - 1 - y)

    in_copies = [pltpu.make_async_copy(src.at[0], dst, in_sems.at[n]) for n, (src, dst) in enumerate(((h_init, out0), (c_init, cio)))]
    for copy in in_copies:
        copy.start()
    w_copies = []
    for d in range(3):
        kd = jnp.where(core == 0, d, 2 - d)
        first = 4 * LANES * d
        pieces = [(first + LANES * dx, dx, 0, LANES) for dx in range(3)] + [(first + 3 * LANES + HALF * dx, dx, LANES, HALF) for dx in range(2)]
        for dst, dx, ch, size in pieces + [(12 * LANES + HALF * d, 2, LANES, HALF)]:
            w_copies.append(pltpu.make_async_copy(w_hbm.at[kd, dx, pl.ds(ch, size)], ws_ref.at[pl.ds(dst, size)], w_sems.at[len(w_copies)]))
    for copy in w_copies:
        copy.start()

    for ref in (fa0, fb0, fa1, fb1):
        ref[0:PITCH, :] = jnp.zeros((PITCH, LANES), F32)
        ref[(GROWS - 2) * PITCH:, :] = jnp.zeros((2 * PITCH, LANES), F32)
    for ref in (hb0, hb1):
        ref[0] = jnp.zeros((COLS, WIDTH), BF16)
    ws_ref[DEPTH - HALF:, :] = jnp.zeros((HALF, GATES), BF16)
    for ref in (el, er, from_left, from_right, diag_left, diag_right):
        ref[...] = jnp.zeros(ref.shape, F32)

    barrier = pltpu.get_barrier_semaphore()
    pl.semaphore_signal(barrier, inc=1, device_id={"rows": other}, device_id_type=MESH)
    for there, near in ((has_left, col - 1), (has_right, col + 1)):
        @pl.when(there)
        def _():
            pl.semaphore_signal(barrier, inc=1, device_id={"cols": near}, device_id_type=MESH)
            pl.semaphore_signal(barrier, inc=1, device_id={"cols": near, "rows": other}, device_id_type=MESH)

    low = lax.broadcasted_iota(jnp.int32, (1, LANES), 1) < HALF
    og_in = jnp.where(low, 0.5, 1.0).astype(F32)
    og_add = jnp.where(low, 0.5, 0.0).astype(F32)

    def sel(a, b):
        return jnp.where(low, a, b)

    def half_turn(x):
        return pltpu.roll(x, HALF, 1)

    def gate_blocks(t):
        return [t[0], half_turn(sel(t[2], t[1])), t[3], half_turn(sel(t[5], t[4])), sel(t[1], t[2]), sel(t[4], t[5])]

    for n, block in enumerate(gate_blocks([bias_ref[:, lanes(n)] for n in range(6)])):
        bp[:, lanes(n)] = block

    pl.semaphore_wait(barrier, 1 + 2 * has_left.astype(jnp.int32) + 2 * has_right.astype(jnp.int32))

    def side_copies(src, to, near, diag, slot, send, near_sem, diag_sem):
        return [
            pltpu.make_async_remote_copy(src, near.at[slot], col_send.at[send], near_sem.at[slot], device_id={"cols": to}, device_id_type=MESH),
            pltpu.make_async_remote_copy(src.at[:, pl.ds(ROWS - 8, 8)], diag.at[slot], col_send.at[send + 1], diag_sem.at[slot], device_id={"cols": to, "rows": other}, device_id_type=MESH),
        ]

    def columns(slot, start):
        def right():
            return side_copies(to_right, col + 1, from_left, diag_left, slot, 0, left_recv, dleft_recv)

        def left():
            return side_copies(to_left, col - 1, from_right, diag_right, slot, 2, right_recv, dright_recv)

        for there, copies, back in ((has_right, right, left), (has_left, left, right)):
            @pl.when(there)
            def _():
                for copy in copies():
                    copy.start() if start else copy.wait_send()
                if not start:
                    for copy in back():
                        copy.wait_recv()

    def seam_copies(slot):
        parts = [(ref, pl.ds(at_row(ROWS - k), COLS)) for k in range(2) for ref in (fa0, fb0)] + [(ref, pl.ds((ROWS - 1) * COLS, COLS)) for ref in (ca, cb)]
        return [
            pltpu.make_async_remote_copy(ref.at[rows], seam.at[slot, n], seam_send.at[n], seam_recv.at[slot, n], device_id={"rows": other}, device_id_type=MESH)
            for n, (ref, rows) in enumerate(parts)
        ]

    def column(ref, x, rows=ROWS):
        return ref[pl.ds(at_row(1) + x, rows, stride=PITCH), :]

    def build_messages():
        for out, a, b, lo, hi, x in ((to_right, 62, 63, 62, 63, 63), (to_left, 0, 1, 1, 0, 0)):
            out[0] = column(fa0, a)
            out[1] = column(fa0, b)
            out[2] = sel(column(fb0, lo), column(fb0, hi))
            out[3] = ca[pl.ds(x, ROWS, stride=COLS), :]
            out[4] = cb[pl.ds(x, ROWS, stride=COLS), :]

    def insert_halos(slot):
        for k in range(2):
            for n, ref in enumerate((fa0, fb0)):
                ref[at_row(ROWS + 1 + k):at_row(ROWS + 1 + k) + COLS, :] = seam[slot, 2 * k + n]
        for n, ref in enumerate((ca, cb)):
            ref[ROWS * COLS:, :] = seam[slot, 4 + n]
        for ext, box, corner, beside, own in ((el, from_left, diag_left, -1, 0), (er, from_right, diag_right, COLS, COLS - 1)):
            parts = [(slice(8, 8 + ROWS), [box[slot, n] for n in range(5)], column(fa0, own), column(fb0, own))]
            for k in range(2):
                cell = at_row(ROWS + 1 + k) + own
                parts.append((slice(8 + ROWS + k, 9 + ROWS + k), [corner[slot, n, 7 - k:8 - k] for n in range(5)], fa0[cell:cell + 1, :], fb0[cell:cell + 1, :]))
            for k, (rows, (a0, a1, p, c_a, c_b), own_a, own_b) in enumerate(parts):
                if beside < 0:
                    tiles = (a0, a1, own_a, p, own_b, c_a, c_b)
                    near = a1
                else:
                    tiles = (own_a, a0, a1, sel(own_b, p), sel(p, half_turn(p)), c_a, c_b)
                    near = a0
                for n, tile in enumerate(tiles):
                    ext[n, rows, :] = tile
                far = sel(half_turn(p), p)
                if k == 0:
                    cells = pl.ds(at_row(1) + beside, ROWS, stride=PITCH)
                else:
                    cells = pl.ds(at_row(ROWS + k) + beside, 1)
                fa0[cells, :] = near
                fb0[cells, :] = far

        def both(n, e):
            return jnp.concatenate([ext[n, 7 + e:7 + e + STRIP, :] for ext in (el, er)], axis=0)

        for e in range(3):
            for n in range(4):
                sb[:, lanes(4 * e + n)] = both(n, e).astype(BF16)
        sb[:, lanes(12)] = sel(both(4, 0), both(4, 1)).astype(BF16)
        sb[:, lanes(13)] = both(4, 2).astype(BF16)

    def put_operands(hb, r, cells, a, b):
        for n in range(3):
            hb[r, cells, lanes(n)] = a[n].astype(BF16)
        hb[r, cells, lanes(3)] = sel(b[0], b[1]).astype(BF16)
        hb[r, cells, lanes(4)] = b[2].astype(BF16)

    def assemble_inner(fa, fb, hb, r):
        at = at_row(r) + EDGE
        a, b = ([ref[at + s:at + s + INNER, :] for s in (-1, 0, 1)] for ref in (fa, fb))
        put_operands(hb, r, slice(0, INNER), a, b)

    def assemble_edge(fa, fb, hb, r):
        at = at_row(r)
        a, b = ([jnp.concatenate([ref[x + s:x + s + EDGE, :] for x in (at, at + COLS - EDGE)], axis=0) for s in (-1, 0, 1)] for ref in (fa, fb))
        put_operands(hb, r, slice(INNER, COLS), a, b)

    def write_out(fa, fb, out, y):
        at = at_row(y + 1)
        row = out_row(y)
        out[row, :, 0:LANES] = fa[at:at + COLS, :].astype(BF16)
        out[row, :, LANES:CH] = fb[at:at + COLS, 0:HALF].astype(BF16)

    def gates(z, bias, c_a, c_b):
        z = [z[:, lanes(n)] + bias[:, lanes(n)] for n in range(6)]
        ca_new = sigmoid(z[1]) * c_a + sigmoid(z[0]) * jnp.tanh(z[3])
        h_a = sigmoid(z[2]) * jnp.tanh(ca_new)
        out_cand = jnp.tanh(z[5] * og_in) * og_in + og_add
        turned = half_turn(out_cand)
        terms = sigmoid(z[4]) * sel(turned, c_b)
        cb_new = terms + half_turn(terms)
        h_b = sel(out_cand, turned) * jnp.tanh(cb_new)
        return h_a, h_b, ca_new, cb_new

    def unit_rows(unit):
        kind, y, count = unit
        return {"I": INNER, "E": 2 * EDGE * count, "S": 2 * STRIP}[kind]

    def unit_lhs(hb, unit):
        kind, y, count = unit
        if kind == "S":
            return sb[...]

        def block(r, part):
            if kind == "I":
                return hb[r, 0:INNER, part]
            return hb[r:r + count, INNER:COLS, part].reshape(unit_rows(unit), part.stop - part.start)

        near = [block(y + e, lanes(0, 4)) for e in range(3)]
        far = [block(y + e, lanes(4)) for e in range(3)]
        return jnp.concatenate(near + [sel(far[0], far[1]), far[2]], axis=1)

    def unit_gates(unit, z, bias, fa, fb):
        kind, y, count = unit
        if kind == "S":
            c_a, c_b = (jnp.concatenate([ext[n, 8:8 + STRIP, :] for ext in (el, er)], axis=0) for n in (5, 6))
            h_a, h_b, _, _ = gates(z, bias, c_a, c_b)
            for beside, first, there in ((-1, 0, has_left), (COLS, STRIP, has_right)):
                for ref, h in ((fa, h_a), (fb, h_b)):
                    h = jnp.where(there, h[first:first + STRIP], 0.0)
                    ref[pl.ds(at_row(1) + beside, ROWS, stride=PITCH), :] = h[0:ROWS]
                    ref[pl.ds(at_row(ROWS + 1) + beside, 1), :] = h[ROWS:ROWS + 1]
            return
        if kind == "I":
            spans = [(y, EDGE, INNER)]
        else:
            spans = [(y + n, x, EDGE) for n in range(count) for x in (0, COLS - EDGE)]
        cells = [slice(r * COLS + x, r * COLS + x + size) for r, x, size in spans]
        c_a, c_b = (jnp.concatenate([ref[part, :] for part in cells], axis=0) for ref in (ca, cb))
        h_a, h_b, ca_new, cb_new = gates(z, bias, c_a, c_b)
        done = 0
        for (r, x, size), part in zip(spans, cells):
            to = slice(at_row(r + 1) + x, at_row(r + 1) + x + size)
            for ref, where, value in ((fa, to, h_a), (fb, to, h_b), (ca, part, ca_new), (cb, part, cb_new)):
                ref[where, :] = value[done:done + size]
            done += size

    i_units = [[("I", y, 1) for y in rows] for rows in I_ROWS]
    e_units = [[("E", y, 3) for y in rows[::3]] for rows in E_ROWS]
    old, new = (fa0, fb0), (fa1, fb1)
    results = [None, None]

    def piece(parity, hb, units, tasks):
        lhs = jnp.concatenate([unit_lhs(hb, unit) for unit in units], axis=0)
        results[parity] = jnp.dot(lhs, w_ref[...], preferred_element_type=F32)
        for task in tasks:
            task()

    def gate_tasks(parity, units, bias, state):
        z = results[parity]
        tasks, first = [], 0
        for unit in units:
            size = unit_rows(unit)
            tasks.append(functools.partial(unit_gates, unit, z[first:first + size], bias, *state))
            first += size
        return tasks

    def inner_tasks(state, hb, rows):
        return [functools.partial(assemble_inner, *state, hb, r) for r in rows]

    def edge_tasks(state, hb, rows):
        return [functools.partial(assemble_edge, *state, hb, r) for r in rows]

    def out_tasks(state, out, rows):
        return [functools.partial(write_out, *state, out, y) for y in rows]

    def out_copy(out, t, n):
        return pltpu.make_async_copy(out, h_seq.at[t, 0], out_sems.at[n])

    for copy in in_copies:
        copy.wait()

    def load_row(y, _):
        row = out_row(y)
        h = out0[row].astype(F32)
        c = cio[row]
        to = pl.ds(pl.multiple_of(at_row(y + 1), 8), COLS)
        cells = pl.ds(pl.multiple_of(y * COLS, COLS), COLS)
        for a, b, where, value in ((fa0, fb0, to, h), (ca, cb, cells, c)):
            a[where, :] = value[:, 0:LANES]
            b[where, :] = jnp.concatenate([value[:, LANES:CH]] * 2, axis=1)
        return 0

    lax.fori_loop(0, ROWS, load_row, 0)
    build_messages()

    def load_weights(n, _):
        rows = pl.ds(pl.multiple_of(n * HALF, HALF), HALF)
        blocks = gate_blocks([ws_ref[rows, lanes(i)].astype(F32) for i in range(6)])
        for i, block in enumerate(blocks):
            w_ref[rows, lanes(i)] = block.astype(BF16)
        return 0

    for copy in w_copies:
        copy.wait()
    columns(0, True)
    for copy in seam_copies(0):
        copy.start()
    lax.fori_loop(0, DEPTH // HALF, load_weights, 0)
    for r in range(1, ROWS + 1):
        assemble_inner(*old, hb0, r)

    def two_steps(s, _):
        slot = lax.rem(s, 2)
        more = s < STEPS // 2 - 1
        bias_a = bp[pl.ds(2 * s, 1), :]
        bias_b = bp[pl.ds(2 * s + 1, 1), :]

        piece(0, hb0, i_units[0], [])
        piece(1, hb0, i_units[1], gate_tasks(0, i_units[0], bias_a, new))
        piece(0, hb0, i_units[2], gate_tasks(1, i_units[1], bias_a, new))
        for copy in seam_copies(slot):
            copy.wait()
        columns(slot, False)

        @pl.when(s > 0)
        def _():
            for n, out in enumerate((out0, out1)):
                out_copy(out, 2 * s - 2 + n, n).wait()

        insert_halos(slot)
        for r in range(1, GROWS):
            assemble_edge(*old, hb0, r)
        for r in range(ROWS + 1, GROWS):
            assemble_inner(*old, hb0, r)
        extra = e_units[0] + [("S", 0, 0), ("E", ROWS, 1)]
        last = i_units[3] + [("I", ROWS, 1)]
        piece(1, hb0, e_units[1], gate_tasks(0, i_units[2], bias_a, new))
        piece(0, hb0, extra, gate_tasks(1, e_units[1], bias_a, new))
        piece(1, hb0, last, gate_tasks(0, extra, bias_a, new) + edge_tasks(new, hb1, range(1, 11)))

        piece(0, hb1, e_units[0], gate_tasks(1, last, bias_a, new) + edge_tasks(new, hb1, range(11, ROWS + 2)))
        piece(1, hb1, e_units[1], gate_tasks(0, e_units[0], bias_b, old) + inner_tasks(new, hb1, range(18, ROWS + 2)))
        piece(0, hb1, i_units[3], gate_tasks(1, e_units[1], bias_b, old) + inner_tasks(new, hb1, range(1, 8)))

        @pl.when(more)
        def _():
            build_messages()
            columns(1 - slot, True)

        piece(1, hb1, i_units[0], gate_tasks(0, i_units[3], bias_b, old) + inner_tasks(new, hb1, range(8, 18)) + inner_tasks(old, hb0, range(19, ROWS + 1)))

        @pl.when(more)
        def _():
            for copy in seam_copies(1 - slot):
                copy.start()

        piece(0, hb1, i_units[1], gate_tasks(1, i_units[0], bias_b, old) + inner_tasks(old, hb0, range(1, 7)) + out_tasks(new, out0, range(ROWS)))
        tail = range(12, 18)
        rest = [y for y in range(ROWS) if y not in tail]
        piece(1, hb1, i_units[2], gate_tasks(0, i_units[1], bias_b, old) + inner_tasks(old, hb0, range(7, 13)) + out_tasks(old, out1, rest))
        for task in gate_tasks(1, i_units[2], bias_b, old) + inner_tasks(old, hb0, range(13, 19)) + out_tasks(old, out1, tail):
            task()
        for n, out in enumerate((out0, out1)):
            out_copy(out, 2 * s + n, n).start()
        return 0

    lax.fori_loop(0, STEPS // 2, two_steps, 0)

    def store_row(y, _):
        cells = pl.ds(pl.multiple_of(y * COLS, COLS), COLS)
        row = out_row(y)
        cio[row, :, 0:LANES] = ca[cells, :]
        cio[row, :, LANES:CH] = cb[cells, 0:HALF]
        return 0

    lax.fori_loop(0, ROWS, store_row, 0)
    c_copy = pltpu.make_async_copy(cio, c_last.at[0], in_sems.at[1])
    c_copy.start()
    for n, out in enumerate((out0, out1)):
        out_copy(out, STEPS - 2 + n, n).wait()
    c_copy.wait()


def solution(mesh):
    def device_fn(h_init, c_init, w_rec, gate_bias):
        hbm = pl.BlockSpec(memory_space=pltpu.HBM)
        vmem = pltpu.VMEM
        dma = pltpu.SemaphoreType.DMA
        tile = (ROWS, COLS, CH)
        edge = (5, ROWS, LANES)
        return pl.pallas_call(
            kernel,
            out_shape=(
                jax.ShapeDtypeStruct((STEPS, 1, *tile), BF16),
                jax.ShapeDtypeStruct((1, *tile), F32),
            ),
            in_specs=[hbm, hbm, hbm, pl.BlockSpec(memory_space=pltpu.VMEM)],
            out_specs=(hbm, hbm),
            scratch_shapes=[
                *[vmem((DEPTH, GATES), BF16)] * 2,
                *[vmem((GROWS * PITCH, LANES), F32)] * 4,
                *[vmem((GROWS, COLS, WIDTH), BF16)] * 2,
                *[vmem(((ROWS + 1) * COLS, LANES), F32)] * 2,
                vmem((2 * STRIP, DEPTH), BF16),
                *[vmem((7, EXT, LANES), F32)] * 2,
                *[vmem(tile, BF16)] * 2,
                vmem(tile, F32),
                vmem((STEPS, GATES), F32),
                *[vmem(edge, F32)] * 2,
                *[vmem((2, *edge), F32)] * 2,
                *[vmem((2, 5, 8, LANES), F32)] * 2,
                vmem((2, 6, COLS, LANES), F32),
                dma((18,)),
                dma((2,)),
                dma((2,)),
                dma((4,)),
                *[dma((2,))] * 4,
                dma((6,)),
                dma((2, 6)),
            ],
            compiler_params=pltpu.CompilerParams(collective_id=0, has_side_effects=True, vmem_limit_bytes=60 * 1024 * 1024),
        )(h_init, c_init, w_rec, gate_bias)

    state_spec = P("dp", "rows", "cols", None)
    return jax.shard_map(device_fn, mesh=mesh, in_specs=(state_spec, state_spec, P(), P()), out_specs=(P(None, "dp", "rows", "cols", None), state_spec), check_vma=False)
```

```python
import functools

import jax
import jax.numpy as jnp
from jax import lax
from jax.experimental import pallas as pl
from jax.experimental.pallas import tpu as pltpu
from jax.sharding import PartitionSpec as P

MESH = pl.DeviceIdType.MESH
F32 = jnp.float32
BF16 = jnp.bfloat16

STEPS = 16
ROWS = 24
COLS = 64
CH = 192
LANES = 128
HALF = 64
EDGE = 8
INNER = 48
PITCH = 80
GROWS = ROWS + 3
GATES = 4 * CH
DEPTH = 14 * LANES
WIDTH = 5 * LANES
EXT = 2 * ROWS
STRIP = 32

I_ROWS = [range(6 * j, 6 * j + 6) for j in range(4)]
EARLY_ROWS = [range(6), range(6, 12), range(12, 17), range(17, 22)]
LATE_ROWS = range(22, ROWS + 1)
E_ROWS = [range(9), range(9, ROWS)]


def lanes(n, count=1):
    return slice(LANES * n, LANES * (n + count))


def sigmoid(x):
    return 0.5 * jnp.tanh(0.5 * x) + 0.5


def at_row(r):
    return r * PITCH + EDGE


def kernel(h_init, c_init, w_hbm, bias_ref, h_seq, c_last, w_ref, ws_ref, fa0, fb0, fa1, fb1, hb0, hb1, ca, cb, sb, el, er,
           out0, out1, cio, bp, zs, to_right, to_left, from_left, from_right, diag_left, diag_right, seam,
           w_sems, in_sems, out_sems, col_send, left_recv, right_recv, dleft_recv, dright_recv, seam_send, seam_recv):
    col_count = lax.axis_size("cols")
    core = lax.axis_index("rows")
    col = lax.axis_index("cols")
    other = 1 - core
    has_left = col > 0
    has_right = col < col_count - 1

    def out_row(y):
        return jnp.where(core == 0, y, ROWS - 1 - y)

    in_copies = [pltpu.make_async_copy(src.at[0], dst, in_sems.at[n]) for n, (src, dst) in enumerate(((h_init, out0), (c_init, cio)))]
    for copy in in_copies:
        copy.start()
    w_copies = []
    for d in range(3):
        kd = jnp.where(core == 0, d, 2 - d)
        first = 4 * LANES * d
        pieces = [(first + LANES * dx, dx, 0, LANES) for dx in range(3)] + [(first + 3 * LANES + HALF * dx, dx, LANES, HALF) for dx in range(2)]
        for dst, dx, ch, size in pieces + [(12 * LANES + HALF * d, 2, LANES, HALF)]:
            w_copies.append(pltpu.make_async_copy(w_hbm.at[kd, dx, pl.ds(ch, size)], ws_ref.at[pl.ds(dst, size)], w_sems.at[len(w_copies)]))
    for copy in w_copies:
        copy.start()

    for ref in (fa0, fb0, fa1, fb1):
        ref[0:PITCH, :] = jnp.zeros((PITCH, LANES), F32)
        ref[(GROWS - 2) * PITCH:, :] = jnp.zeros((2 * PITCH, LANES), F32)
    for ref in (hb0, hb1):
        ref[0] = jnp.zeros((COLS, WIDTH), BF16)
    ws_ref[DEPTH - HALF:, :] = jnp.zeros((HALF, GATES), BF16)
    for ref in (el, er, from_left, from_right, diag_left, diag_right):
        ref[...] = jnp.zeros(ref.shape, F32)

    barrier = pltpu.get_barrier_semaphore()
    pl.semaphore_signal(barrier, inc=1, device_id={"rows": other}, device_id_type=MESH)
    for there, near in ((has_left, col - 1), (has_right, col + 1)):
        @pl.when(there)
        def _():
            pl.semaphore_signal(barrier, inc=1, device_id={"cols": near}, device_id_type=MESH)
            pl.semaphore_signal(barrier, inc=1, device_id={"cols": near, "rows": other}, device_id_type=MESH)

    low = lax.broadcasted_iota(jnp.int32, (1, LANES), 1) < HALF
    og_in = jnp.where(low, 0.5, 1.0).astype(F32)
    og_add = jnp.where(low, 0.5, 0.0).astype(F32)

    def sel(a, b):
        return jnp.where(low, a, b)

    def half_turn(x):
        return pltpu.roll(x, HALF, 1)

    def gate_blocks(t):
        return [t[0], half_turn(sel(t[2], t[1])), t[3], half_turn(sel(t[5], t[4])), sel(t[1], t[2]), sel(t[4], t[5])]

    for n, block in enumerate(gate_blocks([bias_ref[:, lanes(n)] for n in range(6)])):
        bp[:, lanes(n)] = block

    pl.semaphore_wait(barrier, 1 + 2 * has_left.astype(jnp.int32) + 2 * has_right.astype(jnp.int32))

    def side_copies(src, to, near, diag, slot, send, near_sem, diag_sem):
        return [
            pltpu.make_async_remote_copy(src, near.at[slot], col_send.at[send], near_sem.at[slot], device_id={"cols": to}, device_id_type=MESH),
            pltpu.make_async_remote_copy(src.at[:, pl.ds(ROWS - 8, 8)], diag.at[slot], col_send.at[send + 1], diag_sem.at[slot], device_id={"cols": to, "rows": other}, device_id_type=MESH),
        ]

    def columns(slot, start):
        def right():
            return side_copies(to_right, col + 1, from_left, diag_left, slot, 0, left_recv, dleft_recv)

        def left():
            return side_copies(to_left, col - 1, from_right, diag_right, slot, 2, right_recv, dright_recv)

        for there, copies, back in ((has_right, right, left), (has_left, left, right)):
            @pl.when(there)
            def _():
                for copy in copies():
                    copy.start() if start else copy.wait_send()
                if not start:
                    for copy in back():
                        copy.wait_recv()

    def seam_copies(slot):
        parts = [(ref, pl.ds(at_row(ROWS - k), COLS)) for k in range(2) for ref in (fa0, fb0)] + [(ref, pl.ds((ROWS - 1) * COLS, COLS)) for ref in (ca, cb)]
        return [
            pltpu.make_async_remote_copy(ref.at[rows], seam.at[slot, n], seam_send.at[n], seam_recv.at[slot, n], device_id={"rows": other}, device_id_type=MESH)
            for n, (ref, rows) in enumerate(parts)
        ]

    def column(ref, x, rows=ROWS):
        return ref[pl.ds(at_row(1) + x, rows, stride=PITCH), :]

    def build_messages():
        for out, a, b, lo, hi, x in ((to_right, 62, 63, 62, 63, 63), (to_left, 0, 1, 1, 0, 0)):
            out[0] = column(fa0, a)
            out[1] = column(fa0, b)
            out[2] = sel(column(fb0, lo), column(fb0, hi))
            out[3] = ca[pl.ds(x, ROWS, stride=COLS), :]
            out[4] = cb[pl.ds(x, ROWS, stride=COLS), :]

    def insert_halos(slot):
        for k in range(2):
            for n, ref in enumerate((fa0, fb0)):
                ref[at_row(ROWS + 1 + k):at_row(ROWS + 1 + k) + COLS, :] = seam[slot, 2 * k + n]
        for n, ref in enumerate((ca, cb)):
            ref[ROWS * COLS:, :] = seam[slot, 4 + n]
        for ext, box, corner, beside, own in ((el, from_left, diag_left, -1, 0), (er, from_right, diag_right, COLS, COLS - 1)):
            parts = [(slice(8, 8 + ROWS), [box[slot, n] for n in range(5)], column(fa0, own), column(fb0, own))]
            for k in range(2):
                cell = at_row(ROWS + 1 + k) + own
                parts.append((slice(8 + ROWS + k, 9 + ROWS + k), [corner[slot, n, 7 - k:8 - k] for n in range(5)], fa0[cell:cell + 1, :], fb0[cell:cell + 1, :]))
            for k, (rows, (a0, a1, p, c_a, c_b), own_a, own_b) in enumerate(parts):
                if beside < 0:
                    tiles = (a0, a1, own_a, p, own_b, c_a, c_b)
                    near = a1
                else:
                    tiles = (own_a, a0, a1, sel(own_b, p), sel(p, half_turn(p)), c_a, c_b)
                    near = a0
                for n, tile in enumerate(tiles):
                    ext[n, rows, :] = tile
                far = sel(half_turn(p), p)
                if k == 0:
                    cells = pl.ds(at_row(1) + beside, ROWS, stride=PITCH)
                else:
                    cells = pl.ds(at_row(ROWS + k) + beside, 1)
                fa0[cells, :] = near
                fb0[cells, :] = far

    def build_strips():
        def both(n, e):
            return jnp.concatenate([ext[n, 7 + e:7 + e + STRIP, :] for ext in (el, er)], axis=0)

        for e in range(3):
            for n in range(4):
                sb[:, lanes(4 * e + n)] = both(n, e).astype(BF16)
        sb[:, lanes(12)] = sel(both(4, 0), both(4, 1)).astype(BF16)
        sb[:, lanes(13)] = both(4, 2).astype(BF16)

    def put_operands(hb, r, cells, a, b):
        for n in range(3):
            hb[r, cells, lanes(n)] = a[n].astype(BF16)
        hb[r, cells, lanes(3)] = sel(b[0], b[1]).astype(BF16)
        hb[r, cells, lanes(4)] = b[2].astype(BF16)

    def assemble_inner(fa, fb, hb, r):
        at = at_row(r) + EDGE
        a, b = ([ref[at + s:at + s + INNER, :] for s in (-1, 0, 1)] for ref in (fa, fb))
        put_operands(hb, r, slice(0, INNER), a, b)

    def assemble_edge(fa, fb, hb, r):
        at = at_row(r)
        a, b = ([jnp.concatenate([ref[x + s:x + s + EDGE, :] for x in (at, at + COLS - EDGE)], axis=0) for s in (-1, 0, 1)] for ref in (fa, fb))
        put_operands(hb, r, slice(INNER, COLS), a, b)

    def write_out(fa, fb, out, y):
        at = at_row(y + 1)
        row = out_row(y)
        out[row, :, 0:LANES] = fa[at:at + COLS, :].astype(BF16)
        out[row, :, LANES:CH] = fb[at:at + COLS, 0:HALF].astype(BF16)

    def gates(z, bias, c_a, c_b):
        z = [z[:, lanes(n)] + bias[:, lanes(n)] for n in range(6)]
        ca_new = sigmoid(z[1]) * c_a + sigmoid(z[0]) * jnp.tanh(z[3])
        h_a = sigmoid(z[2]) * jnp.tanh(ca_new)
        out_cand = jnp.tanh(z[5] * og_in) * og_in + og_add
        turned = half_turn(out_cand)
        terms = sigmoid(z[4]) * sel(turned, c_b)
        cb_new = terms + half_turn(terms)
        h_b = sel(out_cand, turned) * jnp.tanh(cb_new)
        return h_a, h_b, ca_new, cb_new

    def unit_rows(unit):
        kind, y, count = unit
        return {"I": INNER, "E": 2 * EDGE * count, "S": 2 * STRIP}[kind]

    def unit_lhs(hb, unit):
        kind, y, count = unit
        if kind == "S":
            return sb[...]

        def block(r, part):
            if kind == "I":
                return hb[r, 0:INNER, part]
            return hb[r:r + count, INNER:COLS, part].reshape(unit_rows(unit), part.stop - part.start)

        near = [block(y + e, lanes(0, 4)) for e in range(3)]
        far = [block(y + e, lanes(4)) for e in range(3)]
        return jnp.concatenate(near + [sel(far[0], far[1]), far[2]], axis=1)

    def unit_gates(unit, z, part, bias, fa, fb):
        z = z[part, :]
        kind, y, count = unit
        if kind == "S":
            c_a, c_b = (jnp.concatenate([ext[n, 8:8 + STRIP, :] for ext in (el, er)], axis=0) for n in (5, 6))
            h_a, h_b, _, _ = gates(z, bias, c_a, c_b)
            for beside, first, there in ((-1, 0, has_left), (COLS, STRIP, has_right)):
                for ref, h in ((fa, h_a), (fb, h_b)):
                    h = jnp.where(there, h[first:first + STRIP], 0.0)
                    ref[pl.ds(at_row(1) + beside, ROWS, stride=PITCH), :] = h[0:ROWS]
                    ref[pl.ds(at_row(ROWS + 1) + beside, 1), :] = h[ROWS:ROWS + 1]
            return
        if kind == "I":
            spans = [(y, EDGE, INNER)]
        else:
            spans = [(y + n, x, EDGE) for n in range(count) for x in (0, COLS - EDGE)]
        cells = [slice(r * COLS + x, r * COLS + x + size) for r, x, size in spans]
        c_a, c_b = (jnp.concatenate([ref[part, :] for part in cells], axis=0) for ref in (ca, cb))
        h_a, h_b, ca_new, cb_new = gates(z, bias, c_a, c_b)
        done = 0
        for (r, x, size), part in zip(spans, cells):
            to = slice(at_row(r + 1) + x, at_row(r + 1) + x + size)
            for ref, where, value in ((fa, to, h_a), (fb, to, h_b), (ca, part, ca_new), (cb, part, cb_new)):
                ref[where, :] = value[done:done + size]
            done += size

    def i_units(rows):
        return [("I", y, 1) for y in rows]

    e_units = [[("E", y, 3) for y in rows[::3]] for rows in E_ROWS]
    old, new = (fa0, fb0), (fa1, fb1)
    results = [None, None]

    def piece(parity, hb, units, tasks):
        lhs = jnp.concatenate([unit_lhs(hb, unit) for unit in units], axis=0)
        half = sum(unit_rows(unit) for unit in units[:(len(units) + 1) // 2])
        wide = [jnp.dot(lhs, w_ref[:, lanes(2 * n, 2)], preferred_element_type=F32) for n in range(2)]
        halves = [jnp.dot(part, w_ref[:, lanes(4, 2)], preferred_element_type=F32) for part in (lhs[:half], lhs[half:])]
        results[parity] = jnp.concatenate(wide + [jnp.concatenate(halves, axis=0)], axis=1)
        for task in tasks:
            task()

    def gate_tasks(parity, units, bias, state):
        z = zs if parity is None else results[parity]
        tasks, first = [], 0
        for unit in units:
            size = unit_rows(unit)
            tasks.append(functools.partial(unit_gates, unit, z, slice(first, first + size), bias, *state))
            first += size
        return tasks

    def inner_tasks(state, hb, rows):
        return [functools.partial(assemble_inner, *state, hb, r) for r in rows]

    def edge_tasks(state, hb, rows):
        return [functools.partial(assemble_edge, *state, hb, r) for r in rows]

    def out_tasks(state, out, rows):
        return [functools.partial(write_out, *state, out, y) for y in rows]

    def out_copy(out, t, n):
        return pltpu.make_async_copy(out, h_seq.at[t, 0], out_sems.at[n])

    for copy in in_copies:
        copy.wait()

    def load_row(y, _):
        row = out_row(y)
        h = out0[row].astype(F32)
        c = cio[row]
        to = pl.ds(pl.multiple_of(at_row(y + 1), 8), COLS)
        cells = pl.ds(pl.multiple_of(y * COLS, COLS), COLS)
        for a, b, where, value in ((fa0, fb0, to, h), (ca, cb, cells, c)):
            a[where, :] = value[:, 0:LANES]
            b[where, :] = jnp.concatenate([value[:, LANES:CH]] * 2, axis=1)
        return 0

    lax.fori_loop(0, ROWS, load_row, 0)
    build_messages()

    def load_weights(n, _):
        rows = pl.ds(pl.multiple_of(n * HALF, HALF), HALF)
        blocks = gate_blocks([ws_ref[rows, lanes(i)].astype(F32) for i in range(6)])
        for i, block in enumerate(blocks):
            w_ref[rows, lanes(i)] = block.astype(BF16)
        return 0

    for copy in w_copies:
        copy.wait()
    columns(0, True)
    for copy in seam_copies(0):
        copy.start()
    lax.fori_loop(0, DEPTH // HALF, load_weights, 0)
    for r in range(1, ROWS + 1):
        assemble_inner(*old, hb0, r)

    def bias_of(t):
        return bp[pl.ds(t, 1), :]

    def early(t, tasks):
        units = [i_units(rows) for rows in EARLY_ROWS]
        bias = bias_of(t)
        for n in range(4):
            more = gate_tasks(1 - n % 2, units[n - 1], bias, new) if n else []
            piece(n % 2, hb0, units[n], more + tasks[n])
        zs[...] = results[1]

    def halos(slot):
        for copy in seam_copies(slot):
            copy.wait()
        columns(slot, False)
        insert_halos(slot)

    def rest(s, slot, last):
        bias_a, bias_b = bias_of(2 * s), bias_of(2 * s + 1)
        for r in range(1, 11):
            assemble_edge(*old, hb0, r)

        far = e_units[1] + [("S", 0, 0), ("E", ROWS, 1)]
        late = i_units(LATE_ROWS)
        piece(0, hb0, e_units[0], [build_strips] + edge_tasks(old, hb0, range(11, GROWS)) + gate_tasks(None, i_units(EARLY_ROWS[3]), bias_a, new))
        piece(1, hb0, far, inner_tasks(old, hb0, range(ROWS + 1, GROWS)) + gate_tasks(0, e_units[0], bias_a, new))
        piece(0, hb0, late, gate_tasks(1, far, bias_a, new) + edge_tasks(new, hb1, range(1, 11)))

        rows = [i_units(part) for part in I_ROWS]
        piece(1, hb1, e_units[0], gate_tasks(0, late, bias_a, new) + edge_tasks(new, hb1, range(11, ROWS + 2)))
        piece(0, hb1, e_units[1], gate_tasks(1, e_units[0], bias_b, old) + inner_tasks(new, hb1, range(18, ROWS + 2)))
        piece(1, hb1, rows[3], gate_tasks(0, e_units[1], bias_b, old) + inner_tasks(new, hb1, range(1, 8)))
        piece(0, hb1, rows[0], gate_tasks(1, rows[3], bias_b, old) + inner_tasks(new, hb1, range(8, 18)))
        if not last:
            build_messages()
            columns(1 - slot, True)
            for copy in seam_copies(1 - slot):
                copy.start()

            @pl.when(s > 0)
            def _():
                for n, out in enumerate((out0, out1)):
                    out_copy(out, 2 * s - 2 + n, n).wait()
        else:
            for n, out in enumerate((out0, out1)):
                out_copy(out, 2 * s - 2 + n, n).wait()

        def next_operands(first, count):
            return [] if last else inner_tasks(old, hb0, range(first, first + count))

        piece(1, hb1, rows[1], gate_tasks(0, rows[0], bias_b, old) + next_operands(19, 6) + next_operands(1, 6) + out_tasks(new, out0, range(ROWS)))
        piece(0, hb1, rows[2], gate_tasks(1, rows[1], bias_b, old) + next_operands(7, 6) + out_tasks(old, out1, I_ROWS[0]) + out_tasks(old, out1, I_ROWS[3]))
        tail = gate_tasks(0, rows[2], bias_b, old) + next_operands(13, 6)
        done = out_tasks(old, out1, I_ROWS[1]) + out_tasks(old, out1, I_ROWS[2])
        if last:
            for task in tail + done:
                task()
        else:
            early(2 * s + 2, [tail, done[:6], done[6:], []])
        for n, out in enumerate((out0, out1)):
            out_copy(out, 2 * s + n, n).start()

    early(0, [[], [], [], []])

    def two_steps(s, _):
        slot = lax.rem(s, 2)
        halos(slot)
        rest(s, slot, False)
        return 0

    last_pair = STEPS // 2 - 1
    lax.fori_loop(0, last_pair, two_steps, 0)
    halos(last_pair % 2)
    rest(last_pair, last_pair % 2, True)

    def store_row(y, _):
        cells = pl.ds(pl.multiple_of(y * COLS, COLS), COLS)
        row = out_row(y)
        cio[row, :, 0:LANES] = ca[cells, :]
        cio[row, :, LANES:CH] = cb[cells, 0:HALF]
        return 0

    lax.fori_loop(0, ROWS, store_row, 0)
    c_copy = pltpu.make_async_copy(cio, c_last.at[0], in_sems.at[1])
    c_copy.start()
    for n, out in enumerate((out0, out1)):
        out_copy(out, STEPS - 2 + n, n).wait()
    c_copy.wait()


def solution(mesh):
    def device_fn(h_init, c_init, w_rec, gate_bias):
        hbm = pl.BlockSpec(memory_space=pltpu.HBM)
        vmem = pltpu.VMEM
        dma = pltpu.SemaphoreType.DMA
        tile = (ROWS, COLS, CH)
        edge = (5, ROWS, LANES)
        return pl.pallas_call(
            kernel,
            out_shape=(
                jax.ShapeDtypeStruct((STEPS, 1, *tile), BF16),
                jax.ShapeDtypeStruct((1, *tile), F32),
            ),
            in_specs=[hbm, hbm, hbm, pl.BlockSpec(memory_space=pltpu.VMEM)],
            out_specs=(hbm, hbm),
            scratch_shapes=[
                *[vmem((DEPTH, GATES), BF16)] * 2,
                *[vmem((GROWS * PITCH, LANES), F32)] * 4,
                *[vmem((GROWS, COLS, WIDTH), BF16)] * 2,
                *[vmem(((ROWS + 1) * COLS, LANES), F32)] * 2,
                vmem((2 * STRIP, DEPTH), BF16),
                *[vmem((7, EXT, LANES), F32)] * 2,
                *[vmem(tile, BF16)] * 2,
                vmem(tile, F32),
                vmem((STEPS, GATES), F32),
                vmem((len(EARLY_ROWS[3]) * INNER, GATES), F32),
                *[vmem(edge, F32)] * 2,
                *[vmem((2, *edge), F32)] * 2,
                *[vmem((2, 5, 8, LANES), F32)] * 2,
                vmem((2, 6, COLS, LANES), F32),
                dma((18,)),
                dma((2,)),
                dma((2,)),
                dma((4,)),
                *[dma((2,))] * 4,
                dma((6,)),
                dma((2, 6)),
            ],
            compiler_params=pltpu.CompilerParams(collective_id=0, has_side_effects=True, vmem_limit_bytes=60 * 1024 * 1024),
        )(h_init, c_init, w_rec, gate_bias)

    state_spec = P("dp", "rows", "cols", None)
    return jax.shard_map(device_fn, mesh=mesh, in_specs=(state_spec, state_spec, P(), P()), out_specs=(P(None, "dp", "rows", "cols", None), state_spec), check_vma=False)
```

```python
import functools
from types import SimpleNamespace

import jax
import jax.numpy as jnp
from jax import lax
from jax.experimental import pallas as pl
from jax.experimental.pallas import tpu as pltpu
from jax.sharding import PartitionSpec as P

MESH = pl.DeviceIdType.MESH
F32 = jnp.float32
BF16 = jnp.bfloat16

STEPS = 16
ROWS = 24
COLS = 64
CH = 192
LANES = 128
HALF = 64
EDGE = 8
INNER = 48
PITCH = 80
GROWS = ROWS + 3
GATES = 4 * CH
DEPTH = 14 * LANES
WIDTH = 5 * LANES
EXT = 2 * ROWS
STRIP = 32

I_ROWS = [range(6 * j, 6 * j + 6) for j in range(4)]
EARLY_ROWS = [range(6), range(6, 12), range(12, 17), range(17, 22)]
LATE_ROWS = range(22, ROWS + 1)
E_ROWS = [range(9), range(9, ROWS)]


def lanes(n, count=1):
    return slice(LANES * n, LANES * (n + count))


def sigmoid(x):
    return 0.5 * jnp.tanh(0.5 * x) + 0.5


def at_row(r):
    return r * PITCH + EDGE


STATE = ("hs", "w_ref", "bp", "fa0", "fb0", "fa1", "fb1", "hb0", "ca", "cb", "zs", "el", "er")
FIRST = ("ws_ref", "hin", "cio", "hb1", "sb", "to_right", "to_left", "from_left", "from_right", "diag_left", "diag_right", "seam")
SEMS = ("w_sems", "in_sems", "col_send", "left_recv", "right_recv", "dleft_recv", "dright_recv", "seam_send", "seam_recv")


def exchange_kernel(h_init, c_init, w_hbm, bias_ref, *refs):
    names = STATE + FIRST + SEMS
    work(True, SimpleNamespace(h_init=h_init, c_init=c_init, w_hbm=w_hbm, bias_ref=bias_ref, **dict(zip(names, refs))))


def final_kernel(*refs):
    outs = ("h_seq", "c_last", *["done_" + name for name in CHANGED])
    names = STATE + outs + ("hb1", "sb", "out0", "out1", "cio", "out_sems", "in_sems")
    work(False, SimpleNamespace(**dict(zip(names, refs))))


CHANGED = ("fa0", "fb0", "fa1", "fb1", "hb0", "ca", "cb")


def work(exchange, refs):
    fa0, fb0, fa1, fb1, hb0, hb1, ca, cb = refs.fa0, refs.fb0, refs.fa1, refs.fb1, refs.hb0, refs.hb1, refs.ca, refs.cb
    w_ref, bp, zs, el, er, sb, cio, in_sems = refs.w_ref, refs.bp, refs.zs, refs.el, refs.er, refs.sb, refs.cio, refs.in_sems
    if exchange:
        ws_ref, to_right, to_left, from_left, from_right = refs.ws_ref, refs.to_right, refs.to_left, refs.from_left, refs.from_right
        diag_left, diag_right, seam = refs.diag_left, refs.diag_right, refs.seam
    else:
        fa0, fb0, fa1, fb1, hb0, ca, cb = (getattr(refs, "done_" + name) for name in CHANGED)
    col_count = lax.axis_size("cols")
    core = lax.axis_index("rows")
    col = lax.axis_index("cols")
    other = 1 - core
    has_left = col > 0
    has_right = col < col_count - 1

    def out_row(y):
        return jnp.where(core == 0, y, ROWS - 1 - y)

    low = lax.broadcasted_iota(jnp.int32, (1, LANES), 1) < HALF
    og_in = jnp.where(low, 0.5, 1.0).astype(F32)
    og_add = jnp.where(low, 0.5, 0.0).astype(F32)

    def sel(a, b):
        return jnp.where(low, a, b)

    def half_turn(x):
        return pltpu.roll(x, HALF, 1)

    def gate_blocks(t):
        return [t[0], half_turn(sel(t[2], t[1])), t[3], half_turn(sel(t[5], t[4])), sel(t[1], t[2]), sel(t[4], t[5])]

    def side_copies(src, to, near, diag, slot, send, near_sem, diag_sem):
        return [
            pltpu.make_async_remote_copy(src, near.at[slot], refs.col_send.at[send], near_sem.at[slot], device_id={"cols": to}, device_id_type=MESH),
            pltpu.make_async_remote_copy(src.at[:, pl.ds(ROWS - 8, 8)], diag.at[slot], refs.col_send.at[send + 1], diag_sem.at[slot], device_id={"cols": to, "rows": other}, device_id_type=MESH),
        ]

    def columns(slot, start):
        def right():
            return side_copies(to_right, col + 1, from_left, diag_left, slot, 0, refs.left_recv, refs.dleft_recv)

        def left():
            return side_copies(to_left, col - 1, from_right, diag_right, slot, 2, refs.right_recv, refs.dright_recv)

        for there, copies, back in ((has_right, right, left), (has_left, left, right)):
            @pl.when(there)
            def _():
                for copy in copies():
                    copy.start() if start else copy.wait_send()
                if not start:
                    for copy in back():
                        copy.wait_recv()

    def seam_copies(slot):
        parts = [(ref, pl.ds(at_row(ROWS - k), COLS)) for k in range(2) for ref in (fa0, fb0)] + [(ref, pl.ds((ROWS - 1) * COLS, COLS)) for ref in (ca, cb)]
        return [
            pltpu.make_async_remote_copy(ref.at[rows], seam.at[slot, n], refs.seam_send.at[n], refs.seam_recv.at[slot, n], device_id={"rows": other}, device_id_type=MESH)
            for n, (ref, rows) in enumerate(parts)
        ]

    def column(ref, x, rows=ROWS):
        return ref[pl.ds(at_row(1) + x, rows, stride=PITCH), :]

    def build_messages():
        for out, a, b, lo, hi, x in ((to_right, 62, 63, 62, 63, 63), (to_left, 0, 1, 1, 0, 0)):
            out[0] = column(fa0, a)
            out[1] = column(fa0, b)
            out[2] = sel(column(fb0, lo), column(fb0, hi))
            out[3] = ca[pl.ds(x, ROWS, stride=COLS), :]
            out[4] = cb[pl.ds(x, ROWS, stride=COLS), :]

    def insert_halos(slot):
        for k in range(2):
            for n, ref in enumerate((fa0, fb0)):
                ref[at_row(ROWS + 1 + k):at_row(ROWS + 1 + k) + COLS, :] = seam[slot, 2 * k + n]
        for n, ref in enumerate((ca, cb)):
            ref[ROWS * COLS:, :] = seam[slot, 4 + n]
        for ext, box, corner, beside, own in ((el, from_left, diag_left, -1, 0), (er, from_right, diag_right, COLS, COLS - 1)):
            parts = [(slice(8, 8 + ROWS), [box[slot, n] for n in range(5)], column(fa0, own), column(fb0, own))]
            for k in range(2):
                cell = at_row(ROWS + 1 + k) + own
                parts.append((slice(8 + ROWS + k, 9 + ROWS + k), [corner[slot, n, 7 - k:8 - k] for n in range(5)], fa0[cell:cell + 1, :], fb0[cell:cell + 1, :]))
            for k, (rows, (a0, a1, p, c_a, c_b), own_a, own_b) in enumerate(parts):
                if beside < 0:
                    tiles = (a0, a1, own_a, p, own_b, c_a, c_b)
                    near = a1
                else:
                    tiles = (own_a, a0, a1, sel(own_b, p), sel(p, half_turn(p)), c_a, c_b)
                    near = a0
                for n, tile in enumerate(tiles):
                    ext[n, rows, :] = tile
                far = sel(half_turn(p), p)
                if k == 0:
                    cells = pl.ds(at_row(1) + beside, ROWS, stride=PITCH)
                else:
                    cells = pl.ds(at_row(ROWS + k) + beside, 1)
                fa0[cells, :] = near
                fb0[cells, :] = far

    def build_strips():
        def both(n, e):
            return jnp.concatenate([ext[n, 7 + e:7 + e + STRIP, :] for ext in (el, er)], axis=0)

        for e in range(3):
            for n in range(4):
                sb[:, lanes(4 * e + n)] = both(n, e).astype(BF16)
        sb[:, lanes(12)] = sel(both(4, 0), both(4, 1)).astype(BF16)
        sb[:, lanes(13)] = both(4, 2).astype(BF16)

    def put_operands(hb, r, cells, a, b):
        for n in range(3):
            hb[r, cells, lanes(n)] = a[n].astype(BF16)
        hb[r, cells, lanes(3)] = sel(b[0], b[1]).astype(BF16)
        hb[r, cells, lanes(4)] = b[2].astype(BF16)

    def assemble_inner(fa, fb, hb, r):
        at = at_row(r) + EDGE
        a, b = ([ref[at + s:at + s + INNER, :] for s in (-1, 0, 1)] for ref in (fa, fb))
        put_operands(hb, r, slice(0, INNER), a, b)

    def assemble_edge(fa, fb, hb, r):
        at = at_row(r)
        a, b = ([jnp.concatenate([ref[x + s:x + s + EDGE, :] for x in (at, at + COLS - EDGE)], axis=0) for s in (-1, 0, 1)] for ref in (fa, fb))
        put_operands(hb, r, slice(INNER, COLS), a, b)

    def write_out(fa, fb, out, y):
        at = at_row(y + 1)
        row = out_row(y)
        out[row, :, 0:LANES] = fa[at:at + COLS, :].astype(BF16)
        out[row, :, LANES:CH] = fb[at:at + COLS, 0:HALF].astype(BF16)

    def gates(z, bias, c_a, c_b):
        z = [z[:, lanes(n)] + bias[:, lanes(n)] for n in range(6)]
        ca_new = sigmoid(z[1]) * c_a + sigmoid(z[0]) * jnp.tanh(z[3])
        h_a = sigmoid(z[2]) * jnp.tanh(ca_new)
        out_cand = jnp.tanh(z[5] * og_in) * og_in + og_add
        turned = half_turn(out_cand)
        terms = sigmoid(z[4]) * sel(turned, c_b)
        cb_new = terms + half_turn(terms)
        h_b = sel(out_cand, turned) * jnp.tanh(cb_new)
        return h_a, h_b, ca_new, cb_new

    def unit_rows(unit):
        kind, y, count = unit
        return {"I": INNER, "E": 2 * EDGE * count, "S": 2 * STRIP}[kind]

    def unit_lhs(hb, unit):
        kind, y, count = unit
        if kind == "S":
            return sb[...]

        def block(r, part):
            if kind == "I":
                return hb[r, 0:INNER, part]
            return hb[r:r + count, INNER:COLS, part].reshape(unit_rows(unit), part.stop - part.start)

        near = [block(y + e, lanes(0, 4)) for e in range(3)]
        far = [block(y + e, lanes(4)) for e in range(3)]
        return jnp.concatenate(near + [sel(far[0], far[1]), far[2]], axis=1)

    def unit_gates(unit, z, part, bias, fa, fb):
        z = z[part, :]
        kind, y, count = unit
        if kind == "S":
            c_a, c_b = (jnp.concatenate([ext[n, 8:8 + STRIP, :] for ext in (el, er)], axis=0) for n in (5, 6))
            h_a, h_b, _, _ = gates(z, bias, c_a, c_b)
            for beside, first, there in ((-1, 0, has_left), (COLS, STRIP, has_right)):
                for ref, h in ((fa, h_a), (fb, h_b)):
                    h = jnp.where(there, h[first:first + STRIP], 0.0)
                    ref[pl.ds(at_row(1) + beside, ROWS, stride=PITCH), :] = h[0:ROWS]
                    ref[pl.ds(at_row(ROWS + 1) + beside, 1), :] = h[ROWS:ROWS + 1]
            return
        if kind == "I":
            spans = [(y, EDGE, INNER)]
        else:
            spans = [(y + n, x, EDGE) for n in range(count) for x in (0, COLS - EDGE)]
        cells = [slice(r * COLS + x, r * COLS + x + size) for r, x, size in spans]
        c_a, c_b = (jnp.concatenate([ref[part, :] for part in cells], axis=0) for ref in (ca, cb))
        h_a, h_b, ca_new, cb_new = gates(z, bias, c_a, c_b)
        done = 0
        for (r, x, size), part in zip(spans, cells):
            to = slice(at_row(r + 1) + x, at_row(r + 1) + x + size)
            for ref, where, value in ((fa, to, h_a), (fb, to, h_b), (ca, part, ca_new), (cb, part, cb_new)):
                ref[where, :] = value[done:done + size]
            done += size

    def i_units(rows):
        return [("I", y, 1) for y in rows]

    e_units = [[("E", y, 3) for y in rows[::3]] for rows in E_ROWS]
    old, new = (fa0, fb0), (fa1, fb1)
    results = [None, None]

    def piece(parity, hb, units, tasks):
        lhs = jnp.concatenate([unit_lhs(hb, unit) for unit in units], axis=0)
        half = sum(unit_rows(unit) for unit in units[:(len(units) + 1) // 2])
        wide = [jnp.dot(lhs, w_ref[:, lanes(2 * n, 2)], preferred_element_type=F32) for n in range(2)]
        halves = [jnp.dot(part, w_ref[:, lanes(4, 2)], preferred_element_type=F32) for part in (lhs[:half], lhs[half:])]
        results[parity] = jnp.concatenate(wide + [jnp.concatenate(halves, axis=0)], axis=1)
        for task in tasks:
            task()

    def gate_tasks(parity, units, bias, state):
        z = zs if parity is None else results[parity]
        tasks, first = [], 0
        for unit in units:
            size = unit_rows(unit)
            tasks.append(functools.partial(unit_gates, unit, z, slice(first, first + size), bias, *state))
            first += size
        return tasks

    def inner_tasks(state, hb, rows):
        return [functools.partial(assemble_inner, *state, hb, r) for r in rows]

    def edge_tasks(state, hb, rows):
        return [functools.partial(assemble_edge, *state, hb, r) for r in rows]

    def out_tasks(state, out, rows):
        return [functools.partial(write_out, *state, out, y) for y in rows]

    def out_copy(out, t, n):
        return pltpu.make_async_copy(out, refs.h_seq.at[t, 0], refs.out_sems.at[n])

    def bias_of(t):
        return bp[pl.ds(t, 1), :]

    def early(t, tasks):
        units = [i_units(rows) for rows in EARLY_ROWS]
        bias = bias_of(t)
        for n in range(4):
            more = gate_tasks(1 - n % 2, units[n - 1], bias, new) if n else []
            piece(n % 2, hb0, units[n], more + tasks[n])
        zs[...] = results[1]

    def halos(slot):
        for copy in seam_copies(slot):
            copy.wait()
        columns(slot, False)
        insert_halos(slot)

    def rest(s, slot, last):
        bias_a, bias_b = bias_of(2 * s), bias_of(2 * s + 1)
        for r in range(1, 11):
            assemble_edge(*old, hb0, r)

        far = e_units[1] + [("S", 0, 0), ("E", ROWS, 1)]
        late = i_units(LATE_ROWS)
        piece(0, hb0, e_units[0], [build_strips] + edge_tasks(old, hb0, range(11, GROWS)) + gate_tasks(None, i_units(EARLY_ROWS[3]), bias_a, new))
        piece(1, hb0, far, inner_tasks(old, hb0, range(ROWS + 1, GROWS)) + gate_tasks(0, e_units[0], bias_a, new))
        piece(0, hb0, late, gate_tasks(1, far, bias_a, new) + edge_tasks(new, hb1, range(1, 11)))

        rows = [i_units(part) for part in I_ROWS]
        piece(1, hb1, e_units[0], gate_tasks(0, late, bias_a, new) + edge_tasks(new, hb1, range(11, ROWS + 2)))
        piece(0, hb1, e_units[1], gate_tasks(1, e_units[0], bias_b, old) + inner_tasks(new, hb1, range(18, ROWS + 2)))
        piece(1, hb1, rows[3], gate_tasks(0, e_units[1], bias_b, old) + inner_tasks(new, hb1, range(1, 8)))
        if not last:
            build_messages()
            columns(1 - slot, True)
        piece(0, hb1, rows[0], gate_tasks(1, rows[3], bias_b, old) + inner_tasks(new, hb1, range(8, 18)))
        if not last:
            for copy in seam_copies(1 - slot):
                copy.start()
        out0, out1 = (refs.out0, refs.out1) if last else (refs.hs.at[2 * s], refs.hs.at[2 * s + 1])

        def next_operands(first, count):
            return [] if last else inner_tasks(old, hb0, range(first, first + count))

        piece(1, hb1, rows[1], gate_tasks(0, rows[0], bias_b, old) + next_operands(19, 6) + next_operands(1, 6) + out_tasks(new, out0, range(ROWS)))
        piece(0, hb1, rows[2], gate_tasks(1, rows[1], bias_b, old) + next_operands(7, 6) + out_tasks(old, out1, I_ROWS[0]) + out_tasks(old, out1, I_ROWS[3]))
        tail = gate_tasks(0, rows[2], bias_b, old) + next_operands(13, 6)
        done = out_tasks(old, out1, I_ROWS[1]) + out_tasks(old, out1, I_ROWS[2])
        if last:
            for task in tail + done:
                task()
        else:
            early(2 * s + 2, [tail, done[:6], done[6:], []])
        if last:
            for n, out in enumerate((out0, out1)):
                out_copy(out, 2 * s + n, n).start()

    last_pair = STEPS // 2 - 1
    hb1[0] = jnp.zeros((COLS, WIDTH), BF16)
    if exchange:
        in_copies = [pltpu.make_async_copy(src.at[0], dst, in_sems.at[n]) for n, (src, dst) in enumerate(((refs.h_init, refs.hin), (refs.c_init, cio)))]
        for copy in in_copies:
            copy.start()
        w_copies = []
        for d in range(3):
            kd = jnp.where(core == 0, d, 2 - d)
            first = 4 * LANES * d
            pieces = [(first + LANES * dx, dx, 0, LANES) for dx in range(3)] + [(first + 3 * LANES + HALF * dx, dx, LANES, HALF) for dx in range(2)]
            for dst, dx, ch, size in pieces + [(12 * LANES + HALF * d, 2, LANES, HALF)]:
                w_copies.append(pltpu.make_async_copy(refs.w_hbm.at[kd, dx, pl.ds(ch, size)], ws_ref.at[pl.ds(dst, size)], refs.w_sems.at[len(w_copies)]))
        for copy in w_copies:
            copy.start()

        for ref in (fa0, fb0, fa1, fb1):
            ref[0:PITCH, :] = jnp.zeros((PITCH, LANES), F32)
            ref[(GROWS - 2) * PITCH:, :] = jnp.zeros((2 * PITCH, LANES), F32)
        hb0[0] = jnp.zeros((COLS, WIDTH), BF16)
        ws_ref[DEPTH - HALF:, :] = jnp.zeros((HALF, GATES), BF16)
        for ref in (el, er, from_left, from_right, diag_left, diag_right):
            ref[...] = jnp.zeros(ref.shape, F32)

        barrier = pltpu.get_barrier_semaphore()
        pl.semaphore_signal(barrier, inc=1, device_id={"rows": other}, device_id_type=MESH)
        for there, near in ((has_left, col - 1), (has_right, col + 1)):
            @pl.when(there)
            def _():
                pl.semaphore_signal(barrier, inc=1, device_id={"cols": near}, device_id_type=MESH)
                pl.semaphore_signal(barrier, inc=1, device_id={"cols": near, "rows": other}, device_id_type=MESH)

        for n, block in enumerate(gate_blocks([refs.bias_ref[:, lanes(n)] for n in range(6)])):
            bp[:, lanes(n)] = block

        pl.semaphore_wait(barrier, 1 + 2 * has_left.astype(jnp.int32) + 2 * has_right.astype(jnp.int32))

        for copy in in_copies:
            copy.wait()

        def load_row(y, _):
            row = out_row(y)
            h = refs.hin[row].astype(F32)
            c = cio[row]
            to = pl.ds(pl.multiple_of(at_row(y + 1), 8), COLS)
            cells = pl.ds(pl.multiple_of(y * COLS, COLS), COLS)
            for a, b, where, value in ((fa0, fb0, to, h), (ca, cb, cells, c)):
                a[where, :] = value[:, 0:LANES]
                b[where, :] = jnp.concatenate([value[:, LANES:CH]] * 2, axis=1)
            return 0

        lax.fori_loop(0, ROWS, load_row, 0)
        build_messages()

        def load_weights(n, _):
            rows = pl.ds(pl.multiple_of(n * HALF, HALF), HALF)
            blocks = gate_blocks([ws_ref[rows, lanes(i)].astype(F32) for i in range(6)])
            for i, block in enumerate(blocks):
                w_ref[rows, lanes(i)] = block.astype(BF16)
            return 0

        for copy in w_copies:
            copy.wait()
        columns(0, True)
        for copy in seam_copies(0):
            copy.start()
        lax.fori_loop(0, DEPTH // HALF, load_weights, 0)
        for r in range(1, ROWS + 1):
            assemble_inner(*old, hb0, r)
        early(0, [[], [], [], []])

        def two_steps(s, _):
            slot = lax.rem(s, 2)
            halos(slot)
            rest(s, slot, False)
            return 0

        lax.fori_loop(0, last_pair, two_steps, 0)
        halos(last_pair % 2)
        return

    before = pltpu.make_async_copy(refs.hs, refs.h_seq.at[pl.ds(0, STEPS - 2), 0], refs.out_sems.at[2])
    before.start()
    rest(last_pair, None, True)

    def store_row(y, _):
        cells = pl.ds(pl.multiple_of(y * COLS, COLS), COLS)
        row = out_row(y)
        cio[row, :, 0:LANES] = ca[cells, :]
        cio[row, :, LANES:CH] = cb[cells, 0:HALF]
        return 0

    lax.fori_loop(0, ROWS, store_row, 0)
    c_copy = pltpu.make_async_copy(cio, refs.c_last.at[0], in_sems.at[1])
    c_copy.start()
    before.wait()
    for n, out in enumerate((refs.out0, refs.out1)):
        out_copy(out, STEPS - 2 + n, n).wait()
    c_copy.wait()


def solution(mesh):
    def device_fn(h_init, c_init, w_rec, gate_bias):
        hbm = pl.BlockSpec(memory_space=pltpu.HBM)
        in_vmem = pl.BlockSpec(memory_space=pltpu.VMEM)
        vmem = pltpu.VMEM
        dma = pltpu.SemaphoreType.DMA
        tile = (ROWS, COLS, CH)
        edge = (5, ROWS, LANES)
        operands = vmem((GROWS, COLS, WIDTH), BF16)
        strips = vmem((2 * STRIP, DEPTH), BF16)
        state = dict(
            hs=vmem((STEPS - 2, *tile), BF16),
            w_ref=vmem((DEPTH, GATES), BF16),
            bp=vmem((STEPS, GATES), F32),
            **{name: vmem((GROWS * PITCH, LANES), F32) for name in ("fa0", "fb0", "fa1", "fb1")},
            hb0=operands,
            **{name: vmem(((ROWS + 1) * COLS, LANES), F32) for name in ("ca", "cb")},
            zs=vmem((len(EARLY_ROWS[3]) * INNER, GATES), F32),
            **{name: vmem((7, EXT, LANES), F32) for name in ("el", "er")},
        )
        held = pl.pallas_call(
            exchange_kernel,
            out_shape=tuple(state[name] for name in STATE),
            in_specs=[hbm, hbm, hbm, in_vmem],
            out_specs=(in_vmem,) * len(STATE),
            scratch_shapes=[
                vmem((DEPTH, GATES), BF16),
                vmem(tile, BF16),
                vmem(tile, F32),
                operands,
                strips,
                *[vmem(edge, F32)] * 2,
                *[vmem((2, *edge), F32)] * 2,
                *[vmem((2, 5, 8, LANES), F32)] * 2,
                vmem((2, 6, COLS, LANES), F32),
                dma((18,)),
                dma((2,)),
                dma((4,)),
                *[dma((2,))] * 4,
                dma((6,)),
                dma((2, 6)),
            ],
            compiler_params=pltpu.CompilerParams(collective_id=0, has_side_effects=True, vmem_limit_bytes=41 * 1024 * 1024),
        )(h_init, c_init, w_rec, gate_bias)
        outs = pl.pallas_call(
            final_kernel,
            out_shape=(
                jax.ShapeDtypeStruct((STEPS, 1, *tile), BF16),
                jax.ShapeDtypeStruct((1, *tile), F32),
                *[state[name] for name in CHANGED],
            ),
            in_specs=[in_vmem] * len(STATE),
            out_specs=(hbm, hbm, *[in_vmem] * len(CHANGED)),
            input_output_aliases={STATE.index(name): 2 + n for n, name in enumerate(CHANGED)},
            scratch_shapes=[operands, strips, vmem(tile, BF16), vmem(tile, BF16), vmem(tile, F32), dma((3,)), dma((2,))],
            compiler_params=pltpu.CompilerParams(vmem_limit_bytes=16 * 1024 * 1024),
        )(*held)
        return outs[0], outs[1]

    state_spec = P("dp", "rows", "cols", None)
    return jax.shard_map(device_fn, mesh=mesh, in_specs=(state_spec, state_spec, P(), P()), out_specs=(P(None, "dp", "rows", "cols", None), state_spec), check_vma=False)
```

```python
import functools
from types import SimpleNamespace

import jax
import jax.numpy as jnp
from jax import lax
from jax.experimental import pallas as pl
from jax.experimental.pallas import tpu as pltpu
from jax.sharding import PartitionSpec as P

MESH = pl.DeviceIdType.MESH
F32 = jnp.float32
BF16 = jnp.bfloat16

STEPS = 16
ROWS = 24
COLS = 64
CH = 192
LANES = 128
HALF = 64
EDGE = 8
INNER = 48
PITCH = 80
GROWS = ROWS + 3
GATES = 4 * CH
DEPTH = 14 * LANES
WIDTH = 5 * LANES
EXT = 2 * ROWS
STRIP = 32
CUTS = 4

I_ROWS = [range(6 * j, 6 * j + 6) for j in range(4)]
EARLY_ROWS = [range(6), range(6, 12), range(12, 17), range(17, 22)]
LATE_ROWS = range(22, ROWS + 1)
E_ROWS = [range(9), range(9, ROWS)]


def lanes(n, count=1):
    return slice(LANES * n, LANES * (n + count))


def sigmoid(x):
    return 0.5 * jnp.tanh(0.5 * x) + 0.5


def at_row(r):
    return r * PITCH + EDGE


STATE = ("hs", "w_ref", "bp", "fa0", "fb0", "fa1", "fb1", "hb0", "ca", "cb", "zs", "el", "er")
FIRST = ("ws_ref", "hin", "cio", "hb1", "sb", "to_right", "to_left", "from_left", "from_right", "diag_left", "diag_right", "seam")
SEMS = ("w_sems", "in_sems", "col_send", "left_recv", "right_recv", "dleft_recv", "dright_recv", "seam_send", "seam_recv")


def exchange_kernel(h_init, c_init, w_hbm, bias_ref, *refs):
    names = STATE + FIRST + SEMS
    work(True, SimpleNamespace(h_init=h_init, c_init=c_init, w_hbm=w_hbm, bias_ref=bias_ref, **dict(zip(names, refs))))


def final_kernel(*refs):
    outs = ("h_seq", "c_last", *["done_" + name for name in CHANGED])
    names = STATE + outs + ("hb1", "sb", "out0", "out1", "cio", "step_sems", "out_sems", "in_sems")
    work(False, SimpleNamespace(**dict(zip(names, refs))))


CHANGED = ("fa0", "fb0", "fa1", "fb1", "hb0", "ca", "cb")


def cut_copy(src, dst, sems):
    size = ROWS // CUTS
    return [pltpu.make_async_copy(src.at[pl.ds(size * k, size)], dst.at[pl.ds(size * k, size)], sems.at[k]) for k in range(CUTS)]


def work(exchange, refs):
    fa0, fb0, fa1, fb1, hb0, hb1, ca, cb = refs.fa0, refs.fb0, refs.fa1, refs.fb1, refs.hb0, refs.hb1, refs.ca, refs.cb
    w_ref, bp, zs, el, er, sb, cio, in_sems = refs.w_ref, refs.bp, refs.zs, refs.el, refs.er, refs.sb, refs.cio, refs.in_sems
    if exchange:
        ws_ref, to_right, to_left, from_left, from_right = refs.ws_ref, refs.to_right, refs.to_left, refs.from_left, refs.from_right
        diag_left, diag_right, seam = refs.diag_left, refs.diag_right, refs.seam
    else:
        fa0, fb0, fa1, fb1, hb0, ca, cb = (getattr(refs, "done_" + name) for name in CHANGED)
    col_count = lax.axis_size("cols")
    core = lax.axis_index("rows")
    col = lax.axis_index("cols")
    other = 1 - core
    has_left = col > 0
    has_right = col < col_count - 1

    def out_row(y):
        return jnp.where(core == 0, y, ROWS - 1 - y)

    low = lax.broadcasted_iota(jnp.int32, (1, LANES), 1) < HALF
    og_in = jnp.where(low, 0.5, 1.0).astype(F32)
    og_add = jnp.where(low, 0.5, 0.0).astype(F32)

    def sel(a, b):
        return jnp.where(low, a, b)

    def half_turn(x):
        return pltpu.roll(x, HALF, 1)

    def gate_blocks(t):
        return [t[0], half_turn(sel(t[2], t[1])), t[3], half_turn(sel(t[5], t[4])), sel(t[1], t[2]), sel(t[4], t[5])]

    def side_copies(src, to, near, diag, slot, send, near_sem, diag_sem):
        return [
            pltpu.make_async_remote_copy(src, near.at[slot], refs.col_send.at[send], near_sem.at[slot], device_id={"cols": to}, device_id_type=MESH),
            pltpu.make_async_remote_copy(src.at[:, pl.ds(ROWS - 8, 8)], diag.at[slot], refs.col_send.at[send + 1], diag_sem.at[slot], device_id={"cols": to, "rows": other}, device_id_type=MESH),
        ]

    def columns(slot, start):
        def right():
            return side_copies(to_right, col + 1, from_left, diag_left, slot, 0, refs.left_recv, refs.dleft_recv)

        def left():
            return side_copies(to_left, col - 1, from_right, diag_right, slot, 2, refs.right_recv, refs.dright_recv)

        for there, copies, back in ((has_right, right, left), (has_left, left, right)):
            @pl.when(there)
            def _():
                for copy in copies():
                    copy.start() if start else copy.wait_send()
                if not start:
                    for copy in back():
                        copy.wait_recv()

    def seam_copies(slot):
        parts = [(ref, pl.ds(at_row(ROWS - k), COLS)) for k in range(2) for ref in (fa0, fb0)] + [(ref, pl.ds((ROWS - 1) * COLS, COLS)) for ref in (ca, cb)]
        return [
            pltpu.make_async_remote_copy(ref.at[rows], seam.at[slot, n], refs.seam_send.at[n], refs.seam_recv.at[slot, n], device_id={"rows": other}, device_id_type=MESH)
            for n, (ref, rows) in enumerate(parts)
        ]

    def column(ref, x, rows=ROWS):
        return ref[pl.ds(at_row(1) + x, rows, stride=PITCH), :]

    def build_messages():
        for out, a, b, lo, hi, x in ((to_right, 62, 63, 62, 63, 63), (to_left, 0, 1, 1, 0, 0)):
            out[0] = column(fa0, a)
            out[1] = column(fa0, b)
            out[2] = sel(column(fb0, lo), column(fb0, hi))
            out[3] = ca[pl.ds(x, ROWS, stride=COLS), :]
            out[4] = cb[pl.ds(x, ROWS, stride=COLS), :]

    def insert_halos(slot):
        for k in range(2):
            for n, ref in enumerate((fa0, fb0)):
                ref[at_row(ROWS + 1 + k):at_row(ROWS + 1 + k) + COLS, :] = seam[slot, 2 * k + n]
        for n, ref in enumerate((ca, cb)):
            ref[ROWS * COLS:, :] = seam[slot, 4 + n]
        for ext, box, corner, beside, own in ((el, from_left, diag_left, -1, 0), (er, from_right, diag_right, COLS, COLS - 1)):
            parts = [(slice(8, 8 + ROWS), [box[slot, n] for n in range(5)], column(fa0, own), column(fb0, own))]
            for k in range(2):
                cell = at_row(ROWS + 1 + k) + own
                parts.append((slice(8 + ROWS + k, 9 + ROWS + k), [corner[slot, n, 7 - k:8 - k] for n in range(5)], fa0[cell:cell + 1, :], fb0[cell:cell + 1, :]))
            for k, (rows, (a0, a1, p, c_a, c_b), own_a, own_b) in enumerate(parts):
                if beside < 0:
                    tiles = (a0, a1, own_a, p, own_b, c_a, c_b)
                    near = a1
                else:
                    tiles = (own_a, a0, a1, sel(own_b, p), sel(p, half_turn(p)), c_a, c_b)
                    near = a0
                for n, tile in enumerate(tiles):
                    ext[n, rows, :] = tile
                far = sel(half_turn(p), p)
                if k == 0:
                    cells = pl.ds(at_row(1) + beside, ROWS, stride=PITCH)
                else:
                    cells = pl.ds(at_row(ROWS + k) + beside, 1)
                fa0[cells, :] = near
                fb0[cells, :] = far

    def build_strips():
        def both(n, e):
            return jnp.concatenate([ext[n, 7 + e:7 + e + STRIP, :] for ext in (el, er)], axis=0)

        for e in range(3):
            for n in range(4):
                sb[:, lanes(4 * e + n)] = both(n, e).astype(BF16)
        sb[:, lanes(12)] = sel(both(4, 0), both(4, 1)).astype(BF16)
        sb[:, lanes(13)] = both(4, 2).astype(BF16)

    def put_operands(hb, r, cells, a, b):
        for n in range(3):
            hb[r, cells, lanes(n)] = a[n].astype(BF16)
        hb[r, cells, lanes(3)] = sel(b[0], b[1]).astype(BF16)
        hb[r, cells, lanes(4)] = b[2].astype(BF16)

    def assemble_inner(fa, fb, hb, r):
        at = at_row(r) + EDGE
        a, b = ([ref[at + s:at + s + INNER, :] for s in (-1, 0, 1)] for ref in (fa, fb))
        put_operands(hb, r, slice(0, INNER), a, b)

    def assemble_edge(fa, fb, hb, r):
        at = at_row(r)
        a, b = ([jnp.concatenate([ref[x + s:x + s + EDGE, :] for x in (at, at + COLS - EDGE)], axis=0) for s in (-1, 0, 1)] for ref in (fa, fb))
        put_operands(hb, r, slice(INNER, COLS), a, b)

    def write_out(fa, fb, out, y):
        at = at_row(y + 1)
        row = out_row(y)
        out[row, :, 0:LANES] = fa[at:at + COLS, :].astype(BF16)
        out[row, :, LANES:CH] = fb[at:at + COLS, 0:HALF].astype(BF16)

    def gates(z, bias, c_a, c_b):
        z = [z[:, lanes(n)] + bias[:, lanes(n)] for n in range(6)]
        ca_new = sigmoid(z[1]) * c_a + sigmoid(z[0]) * jnp.tanh(z[3])
        h_a = sigmoid(z[2]) * jnp.tanh(ca_new)
        out_cand = jnp.tanh(z[5] * og_in) * og_in + og_add
        turned = half_turn(out_cand)
        terms = sigmoid(z[4]) * sel(turned, c_b)
        cb_new = terms + half_turn(terms)
        h_b = sel(out_cand, turned) * jnp.tanh(cb_new)
        return h_a, h_b, ca_new, cb_new

    def unit_rows(unit):
        kind, y, count = unit
        return {"I": INNER, "E": 2 * EDGE * count, "S": 2 * STRIP}[kind]

    def unit_lhs(hb, unit):
        kind, y, count = unit
        if kind == "S":
            return sb[...]

        def block(r, part):
            if kind == "I":
                return hb[r, 0:INNER, part]
            return hb[r:r + count, INNER:COLS, part].reshape(unit_rows(unit), part.stop - part.start)

        near = [block(y + e, lanes(0, 4)) for e in range(3)]
        far = [block(y + e, lanes(4)) for e in range(3)]
        return jnp.concatenate(near + [sel(far[0], far[1]), far[2]], axis=1)

    def unit_gates(unit, z, part, bias, fa, fb):
        z = z[part, :]
        kind, y, count = unit
        if kind == "S":
            c_a, c_b = (jnp.concatenate([ext[n, 8:8 + STRIP, :] for ext in (el, er)], axis=0) for n in (5, 6))
            h_a, h_b, _, _ = gates(z, bias, c_a, c_b)
            for beside, first, there in ((-1, 0, has_left), (COLS, STRIP, has_right)):
                for ref, h in ((fa, h_a), (fb, h_b)):
                    h = jnp.where(there, h[first:first + STRIP], 0.0)
                    ref[pl.ds(at_row(1) + beside, ROWS, stride=PITCH), :] = h[0:ROWS]
                    ref[pl.ds(at_row(ROWS + 1) + beside, 1), :] = h[ROWS:ROWS + 1]
            return
        if kind == "I":
            spans = [(y, EDGE, INNER)]
        else:
            spans = [(y + n, x, EDGE) for n in range(count) for x in (0, COLS - EDGE)]
        cells = [slice(r * COLS + x, r * COLS + x + size) for r, x, size in spans]
        c_a, c_b = (jnp.concatenate([ref[part, :] for part in cells], axis=0) for ref in (ca, cb))
        h_a, h_b, ca_new, cb_new = gates(z, bias, c_a, c_b)
        done = 0
        for (r, x, size), part in zip(spans, cells):
            to = slice(at_row(r + 1) + x, at_row(r + 1) + x + size)
            for ref, where, value in ((fa, to, h_a), (fb, to, h_b), (ca, part, ca_new), (cb, part, cb_new)):
                ref[where, :] = value[done:done + size]
            done += size

    def i_units(rows):
        return [("I", y, 1) for y in rows]

    e_units = [[("E", y, 3) for y in rows[::3]] for rows in E_ROWS]
    old, new = (fa0, fb0), (fa1, fb1)
    results = [None, None]

    def piece(parity, hb, units, tasks):
        lhs = jnp.concatenate([unit_lhs(hb, unit) for unit in units], axis=0)
        if exchange:
            results[parity] = jnp.dot(lhs, w_ref[...], preferred_element_type=F32)
        else:
            half = sum(unit_rows(unit) for unit in units[:(len(units) + 1) // 2])
            wide = [jnp.dot(lhs, w_ref[:, lanes(2 * n, 2)], preferred_element_type=F32) for n in range(2)]
            halves = [jnp.dot(part, w_ref[:, lanes(4, 2)], preferred_element_type=F32) for part in (lhs[:half], lhs[half:])]
            results[parity] = jnp.concatenate(wide + [jnp.concatenate(halves, axis=0)], axis=1)
        for task in tasks:
            task()

    def gate_tasks(parity, units, bias, state):
        z = zs if parity is None else results[parity]
        tasks, first = [], 0
        for unit in units:
            size = unit_rows(unit)
            tasks.append(functools.partial(unit_gates, unit, z, slice(first, first + size), bias, *state))
            first += size
        return tasks

    def inner_tasks(state, hb, rows):
        return [functools.partial(assemble_inner, *state, hb, r) for r in rows]

    def edge_tasks(state, hb, rows):
        return [functools.partial(assemble_edge, *state, hb, r) for r in rows]

    def out_tasks(state, out, rows):
        return [functools.partial(write_out, *state, out, y) for y in rows]

    def out_copy(out, t, n):
        return cut_copy(out, refs.h_seq.at[t, 0], refs.out_sems.at[n])

    def bias_of(t):
        return bp[pl.ds(t, 1), :]

    def early(t, tasks):
        units = [i_units(rows) for rows in EARLY_ROWS]
        bias = bias_of(t)
        for n in range(4):
            more = gate_tasks(1 - n % 2, units[n - 1], bias, new) if n else []
            piece(n % 2, hb0, units[n], more + tasks[n])
        zs[...] = results[1]

    def halos(slot):
        for copy in seam_copies(slot):
            copy.wait()
        columns(slot, False)
        insert_halos(slot)

    def rest(s, slot, last):
        bias_a, bias_b = bias_of(2 * s), bias_of(2 * s + 1)
        for r in range(1, 11):
            assemble_edge(*old, hb0, r)

        far = e_units[1] + [("S", 0, 0), ("E", ROWS, 1)]
        late = i_units(LATE_ROWS)
        piece(0, hb0, e_units[0], [build_strips] + edge_tasks(old, hb0, range(11, GROWS)) + gate_tasks(None, i_units(EARLY_ROWS[3]), bias_a, new))
        piece(1, hb0, far, inner_tasks(old, hb0, range(ROWS + 1, GROWS)) + gate_tasks(0, e_units[0], bias_a, new))
        piece(0, hb0, late, gate_tasks(1, far, bias_a, new) + edge_tasks(new, hb1, range(1, 11)))

        rows = [i_units(part) for part in I_ROWS]
        piece(1, hb1, e_units[0], gate_tasks(0, late, bias_a, new) + edge_tasks(new, hb1, range(11, ROWS + 2)))
        piece(0, hb1, e_units[1], gate_tasks(1, e_units[0], bias_b, old) + inner_tasks(new, hb1, range(18, ROWS + 2)))
        piece(1, hb1, rows[3], gate_tasks(0, e_units[1], bias_b, old) + inner_tasks(new, hb1, range(1, 8)))
        if not last:
            build_messages()
            columns(1 - slot, True)
        piece(0, hb1, rows[0], gate_tasks(1, rows[3], bias_b, old) + inner_tasks(new, hb1, range(8, 18)))
        if not last:
            for copy in seam_copies(1 - slot):
                copy.start()
        out0, out1 = (refs.out0, refs.out1) if last else (refs.hs.at[2 * s], refs.hs.at[2 * s + 1])

        def next_operands(first, count):
            return [] if last else inner_tasks(old, hb0, range(first, first + count))

        piece(1, hb1, rows[1], gate_tasks(0, rows[0], bias_b, old) + next_operands(19, 6) + next_operands(1, 6) + out_tasks(new, out0, range(ROWS)))
        piece(0, hb1, rows[2], gate_tasks(1, rows[1], bias_b, old) + next_operands(7, 6) + out_tasks(old, out1, I_ROWS[0]) + out_tasks(old, out1, I_ROWS[3]))
        tail = gate_tasks(0, rows[2], bias_b, old) + next_operands(13, 6)
        done = out_tasks(old, out1, I_ROWS[1]) + out_tasks(old, out1, I_ROWS[2])
        if last:
            for copy in out_copy(out0, 2 * s, 0):
                copy.start()
            for task in tail + done:
                task()
            for copy in out_copy(out1, 2 * s + 1, 1):
                copy.start()
        else:
            early(2 * s + 2, [tail, done[:6], done[6:], []])

    last_pair = STEPS // 2 - 1
    hb1[0] = jnp.zeros((COLS, WIDTH), BF16)
    if exchange:
        in_copies = cut_copy(refs.h_init.at[0], refs.hin, in_sems.at[0]) + cut_copy(refs.c_init.at[0], cio, in_sems.at[1])
        for copy in in_copies:
            copy.start()
        w_copies = []
        for d in range(3):
            kd = jnp.where(core == 0, d, 2 - d)
            first = 4 * LANES * d
            pieces = [(first + LANES * dx, dx, 0, LANES) for dx in range(3)] + [(first + 3 * LANES + HALF * dx, dx, LANES, HALF) for dx in range(2)]
            for dst, dx, ch, size in pieces + [(12 * LANES + HALF * d, 2, LANES, HALF)]:
                w_copies.append(pltpu.make_async_copy(refs.w_hbm.at[kd, dx, pl.ds(ch, size)], ws_ref.at[pl.ds(dst, size)], refs.w_sems.at[len(w_copies)]))
        for copy in w_copies:
            copy.start()

        for ref in (fa0, fb0, fa1, fb1):
            ref[0:PITCH, :] = jnp.zeros((PITCH, LANES), F32)
            ref[(GROWS - 2) * PITCH:, :] = jnp.zeros((2 * PITCH, LANES), F32)
        hb0[0] = jnp.zeros((COLS, WIDTH), BF16)
        ws_ref[DEPTH - HALF:, :] = jnp.zeros((HALF, GATES), BF16)
        for ref in (el, er, from_left, from_right, diag_left, diag_right):
            ref[...] = jnp.zeros(ref.shape, F32)

        barrier = pltpu.get_barrier_semaphore()
        pl.semaphore_signal(barrier, inc=1, device_id={"rows": other}, device_id_type=MESH)
        for there, near in ((has_left, col - 1), (has_right, col + 1)):
            @pl.when(there)
            def _():
                pl.semaphore_signal(barrier, inc=1, device_id={"cols": near}, device_id_type=MESH)
                pl.semaphore_signal(barrier, inc=1, device_id={"cols": near, "rows": other}, device_id_type=MESH)

        for n, block in enumerate(gate_blocks([refs.bias_ref[:, lanes(n)] for n in range(6)])):
            bp[:, lanes(n)] = block


        for copy in in_copies:
            copy.wait()

        def load_rows(n, _):
            for k in range(4):
                y = 4 * n + k
                row = out_row(y)
                to = pl.ds(pl.multiple_of(at_row(y + 1), 8), COLS)
                cells = pl.ds(pl.multiple_of(y * COLS, COLS), COLS)
                for a, b, where, value in ((fa0, fb0, to, refs.hin[row].astype(F32)), (ca, cb, cells, cio[row])):
                    a[where, :] = value[:, 0:LANES]
                    b[where, :] = jnp.concatenate([value[:, LANES:CH]] * 2, axis=1)
            return 0

        lax.fori_loop(0, ROWS // 4, load_rows, 0)
        build_messages()

        def load_weights(n, _):
            rows = pl.ds(pl.multiple_of(n * 4 * HALF, HALF), 4 * HALF)
            blocks = gate_blocks([ws_ref[rows, lanes(i)].astype(F32) for i in range(6)])
            for i, block in enumerate(blocks):
                w_ref[rows, lanes(i)] = block.astype(BF16)
            return 0

        pl.semaphore_wait(barrier, 1 + 2 * has_left.astype(jnp.int32) + 2 * has_right.astype(jnp.int32))
        columns(0, True)
        for copy in seam_copies(0):
            copy.start()
        for copy in w_copies:
            copy.wait()
        lax.fori_loop(0, DEPTH // HALF // 4, load_weights, 0)
        for r in range(1, ROWS + 1):
            assemble_inner(*old, hb0, r)
        early(0, [[], [], [], []])

        def two_steps(s, _):
            slot = lax.rem(s, 2)
            halos(slot)
            rest(s, slot, False)
            return 0

        lax.fori_loop(0, last_pair, two_steps, 0)
        halos(last_pair % 2)
        return

    before = [pltpu.make_async_copy(refs.hs.at[t], refs.h_seq.at[t, 0], refs.step_sems.at[t]) for t in range(STEPS - 2)]
    for copy in before:
        copy.start()
    rest(last_pair, None, True)

    def store_row(y, _):
        cells = pl.ds(pl.multiple_of(y * COLS, COLS), COLS)
        row = out_row(y)
        cio[row, :, 0:LANES] = ca[cells, :]
        cio[row, :, LANES:CH] = cb[cells, 0:HALF]
        return 0

    lax.fori_loop(0, ROWS, store_row, 0)
    c_copies = cut_copy(cio, refs.c_last.at[0], in_sems.at[0])
    for copy in c_copies:
        copy.start()
    for copy in before + out_copy(refs.out0, STEPS - 2, 0) + out_copy(refs.out1, STEPS - 1, 1) + c_copies:
        copy.wait()


def solution(mesh):
    def device_fn(h_init, c_init, w_rec, gate_bias):
        hbm = pl.BlockSpec(memory_space=pltpu.HBM)
        in_vmem = pl.BlockSpec(memory_space=pltpu.VMEM)
        vmem = pltpu.VMEM
        dma = pltpu.SemaphoreType.DMA
        tile = (ROWS, COLS, CH)
        edge = (5, ROWS, LANES)
        operands = vmem((GROWS, COLS, WIDTH), BF16)
        strips = vmem((2 * STRIP, DEPTH), BF16)
        state = dict(
            hs=vmem((STEPS - 2, *tile), BF16),
            w_ref=vmem((DEPTH, GATES), BF16),
            bp=vmem((STEPS, GATES), F32),
            **{name: vmem((GROWS * PITCH, LANES), F32) for name in ("fa0", "fb0", "fa1", "fb1")},
            hb0=operands,
            **{name: vmem(((ROWS + 1) * COLS, LANES), F32) for name in ("ca", "cb")},
            zs=vmem((len(EARLY_ROWS[3]) * INNER, GATES), F32),
            **{name: vmem((7, EXT, LANES), F32) for name in ("el", "er")},
        )
        held = pl.pallas_call(
            exchange_kernel,
            out_shape=tuple(state[name] for name in STATE),
            in_specs=[hbm, hbm, hbm, in_vmem],
            out_specs=(in_vmem,) * len(STATE),
            scratch_shapes=[
                vmem((DEPTH, GATES), BF16),
                vmem(tile, BF16),
                vmem(tile, F32),
                operands,
                strips,
                *[vmem(edge, F32)] * 2,
                *[vmem((2, *edge), F32)] * 2,
                *[vmem((2, 5, 8, LANES), F32)] * 2,
                vmem((2, 6, COLS, LANES), F32),
                dma((18,)),
                dma((2, CUTS)),
                dma((4,)),
                *[dma((2,))] * 4,
                dma((6,)),
                dma((2, 6)),
            ],
            compiler_params=pltpu.CompilerParams(collective_id=0, has_side_effects=True, vmem_limit_bytes=41 * 1024 * 1024),
        )(h_init, c_init, w_rec, gate_bias)
        outs = pl.pallas_call(
            final_kernel,
            out_shape=(
                jax.ShapeDtypeStruct((STEPS, 1, *tile), BF16),
                jax.ShapeDtypeStruct((1, *tile), F32),
                *[state[name] for name in CHANGED],
            ),
            in_specs=[in_vmem] * len(STATE),
            out_specs=(hbm, hbm, *[in_vmem] * len(CHANGED)),
            input_output_aliases={STATE.index(name): 2 + n for n, name in enumerate(CHANGED)},
            scratch_shapes=[operands, strips, vmem(tile, BF16), vmem(tile, BF16), vmem(tile, F32), dma((STEPS - 2,)), dma((2, CUTS)), dma((1, CUTS))],
            compiler_params=pltpu.CompilerParams(vmem_limit_bytes=16 * 1024 * 1024),
        )(*held)
        return outs[0], outs[1]

    state_spec = P("dp", "rows", "cols", None)
    return jax.shard_map(device_fn, mesh=mesh, in_specs=(state_spec, state_spec, P(), P()), out_specs=(P(None, "dp", "rows", "cols", None), state_spec), check_vma=False)
```

```python
import functools
from types import SimpleNamespace

import jax
import jax.numpy as jnp
from jax import lax
from jax.experimental import pallas as pl
from jax.experimental.pallas import tpu as pltpu
from jax.sharding import PartitionSpec as P

MESH = pl.DeviceIdType.MESH
F32 = jnp.float32
BF16 = jnp.bfloat16

STEPS = 16
ROWS = 24
COLS = 64
CH = 192
LANES = 128
HALF = 64
EDGE = 8
INNER = 48
PITCH = 80
GROWS = ROWS + 3
GATES = 4 * CH
DEPTH = 14 * LANES
WIDTH = 5 * LANES
EXT = 2 * ROWS
STRIP = 32
CUTS = 4

I_ROWS = [range(6 * j, 6 * j + 6) for j in range(4)]
EARLY_ROWS = [range(6), range(6, 12), range(12, 17), range(17, 22)]
LATE_ROWS = range(22, ROWS + 1)
E_ROWS = [range(9), range(9, ROWS)]


def lanes(n, count=1):
    return slice(LANES * n, LANES * (n + count))


def sigmoid(x):
    return 0.5 * jnp.tanh(0.5 * x) + 0.5


def at_row(r):
    return r * PITCH + EDGE


STATE = ("hs", "w_ref", "bp", "fa0", "fb0", "fa1", "fb1", "hb0", "ca", "cb", "zs", "el", "er")
FIRST = ("ws_ref", "hin", "cio", "hb1", "sb", "to_right", "to_left", "from_left", "from_right", "diag_left", "diag_right", "seam")
SEMS = ("w_sems", "in_sems", "col_send", "left_recv", "right_recv", "dleft_recv", "dright_recv", "seam_send", "seam_recv")


def exchange_kernel(h_init, c_init, w_hbm, bias_ref, *refs):
    names = STATE + FIRST + SEMS
    work(True, SimpleNamespace(h_init=h_init, c_init=c_init, w_hbm=w_hbm, bias_ref=bias_ref, **dict(zip(names, refs))))


def final_kernel(*refs):
    outs = ("h_seq", "c_last", *["done_" + name for name in CHANGED])
    names = STATE + outs + ("hb1", "sb", "out0", "out1", "cio", "step_sems", "out_sems", "in_sems")
    work(False, SimpleNamespace(**dict(zip(names, refs))))


CHANGED = ("fa0", "fb0", "fa1", "fb1", "hb0", "ca", "cb")


def cut_copy(src, dst, sems):
    size = ROWS // CUTS
    return [pltpu.make_async_copy(src.at[pl.ds(size * k, size)], dst.at[pl.ds(size * k, size)], sems.at[k]) for k in range(CUTS)]


def work(exchange, refs):
    fa0, fb0, fa1, fb1, hb0, hb1, ca, cb = refs.fa0, refs.fb0, refs.fa1, refs.fb1, refs.hb0, refs.hb1, refs.ca, refs.cb
    w_ref, bp, zs, el, er, sb, cio, in_sems = refs.w_ref, refs.bp, refs.zs, refs.el, refs.er, refs.sb, refs.cio, refs.in_sems
    if exchange:
        ws_ref, to_right, to_left, from_left, from_right = refs.ws_ref, refs.to_right, refs.to_left, refs.from_left, refs.from_right
        diag_left, diag_right, seam = refs.diag_left, refs.diag_right, refs.seam
    else:
        fa0, fb0, fa1, fb1, hb0, ca, cb = (getattr(refs, "done_" + name) for name in CHANGED)
    col_count = lax.axis_size("cols")
    core = lax.axis_index("rows")
    col = lax.axis_index("cols")
    other = 1 - core
    has_left = col > 0
    has_right = col < col_count - 1

    def out_row(y):
        return jnp.where(core == 0, y, ROWS - 1 - y)

    low = lax.broadcasted_iota(jnp.int32, (1, LANES), 1) < HALF
    og_in = jnp.where(low, 0.5, 1.0).astype(F32)
    og_add = jnp.where(low, 0.5, 0.0).astype(F32)

    def sel(a, b):
        return jnp.where(low, a, b)

    def half_turn(x):
        return pltpu.roll(x, HALF, 1)

    def gate_blocks(t):
        return [t[0], half_turn(sel(t[2], t[1])), t[3], half_turn(sel(t[5], t[4])), sel(t[1], t[2]), sel(t[4], t[5])]

    def side_copies(src, to, near, diag, slot, send, near_sem, diag_sem):
        return [
            pltpu.make_async_remote_copy(src, near.at[slot], refs.col_send.at[send], near_sem.at[slot], device_id={"cols": to}, device_id_type=MESH),
            pltpu.make_async_remote_copy(src.at[:, pl.ds(ROWS - 8, 8)], diag.at[slot], refs.col_send.at[send + 1], diag_sem.at[slot], device_id={"cols": to, "rows": other}, device_id_type=MESH),
        ]

    def columns(slot, start):
        def right():
            return side_copies(to_right, col + 1, from_left, diag_left, slot, 0, refs.left_recv, refs.dleft_recv)

        def left():
            return side_copies(to_left, col - 1, from_right, diag_right, slot, 2, refs.right_recv, refs.dright_recv)

        for there, copies, back in ((has_right, right, left), (has_left, left, right)):
            @pl.when(there)
            def _():
                for copy in copies():
                    copy.start() if start else copy.wait_send()
                if not start:
                    for copy in back():
                        copy.wait_recv()

    def seam_copies(slot):
        parts = [(ref, pl.ds(at_row(ROWS - k), COLS)) for k in range(2) for ref in (fa0, fb0)] + [(ref, pl.ds((ROWS - 1) * COLS, COLS)) for ref in (ca, cb)]
        return [
            pltpu.make_async_remote_copy(ref.at[rows], seam.at[slot, n], refs.seam_send.at[n], refs.seam_recv.at[slot, n], device_id={"rows": other}, device_id_type=MESH)
            for n, (ref, rows) in enumerate(parts)
        ]

    def column(ref, x, rows=ROWS):
        return ref[pl.ds(at_row(1) + x, rows, stride=PITCH), :]

    def build_messages():
        for out, a, b, lo, hi, x in ((to_right, 62, 63, 62, 63, 63), (to_left, 0, 1, 1, 0, 0)):
            out[0] = column(fa0, a)
            out[1] = column(fa0, b)
            out[2] = sel(column(fb0, lo), column(fb0, hi))
            out[3] = ca[pl.ds(x, ROWS, stride=COLS), :]
            out[4] = cb[pl.ds(x, ROWS, stride=COLS), :]

    def insert_halos(slot):
        for k in range(2):
            for n, ref in enumerate((fa0, fb0)):
                ref[at_row(ROWS + 1 + k):at_row(ROWS + 1 + k) + COLS, :] = seam[slot, 2 * k + n]
        for n, ref in enumerate((ca, cb)):
            ref[ROWS * COLS:, :] = seam[slot, 4 + n]
        for ext, box, corner, beside, own in ((el, from_left, diag_left, -1, 0), (er, from_right, diag_right, COLS, COLS - 1)):
            parts = [(slice(8, 8 + ROWS), [box[slot, n] for n in range(5)], column(fa0, own), column(fb0, own))]
            for k in range(2):
                cell = at_row(ROWS + 1 + k) + own
                parts.append((slice(8 + ROWS + k, 9 + ROWS + k), [corner[slot, n, 7 - k:8 - k] for n in range(5)], fa0[cell:cell + 1, :], fb0[cell:cell + 1, :]))
            for k, (rows, (a0, a1, p, c_a, c_b), own_a, own_b) in enumerate(parts):
                if beside < 0:
                    tiles = (a0, a1, own_a, p, own_b, c_a, c_b)
                    near = a1
                else:
                    tiles = (own_a, a0, a1, sel(own_b, p), sel(p, half_turn(p)), c_a, c_b)
                    near = a0
                for n, tile in enumerate(tiles):
                    ext[n, rows, :] = tile
                far = sel(half_turn(p), p)
                if k == 0:
                    cells = pl.ds(at_row(1) + beside, ROWS, stride=PITCH)
                else:
                    cells = pl.ds(at_row(ROWS + k) + beside, 1)
                fa0[cells, :] = near
                fb0[cells, :] = far

    def build_strips():
        def both(n, e):
            return jnp.concatenate([ext[n, 7 + e:7 + e + STRIP, :] for ext in (el, er)], axis=0)

        for e in range(3):
            for n in range(4):
                sb[:, lanes(4 * e + n)] = both(n, e).astype(BF16)
        sb[:, lanes(12)] = sel(both(4, 0), both(4, 1)).astype(BF16)
        sb[:, lanes(13)] = both(4, 2).astype(BF16)

    def put_operands(hb, r, cells, a, b):
        for n in range(3):
            hb[r, cells, lanes(n)] = a[n].astype(BF16)
        hb[r, cells, lanes(3)] = sel(b[0], b[1]).astype(BF16)
        hb[r, cells, lanes(4)] = b[2].astype(BF16)

    def assemble_inner(fa, fb, hb, r):
        at = at_row(r) + EDGE
        a, b = ([ref[at + s:at + s + INNER, :] for s in (-1, 0, 1)] for ref in (fa, fb))
        put_operands(hb, r, slice(0, INNER), a, b)

    def assemble_edge(fa, fb, hb, r):
        at = at_row(r)
        a, b = ([jnp.concatenate([ref[x + s:x + s + EDGE, :] for x in (at, at + COLS - EDGE)], axis=0) for s in (-1, 0, 1)] for ref in (fa, fb))
        put_operands(hb, r, slice(INNER, COLS), a, b)

    def write_out(fa, fb, out, y):
        at = at_row(y + 1)
        row = out_row(y)
        out[row, :, 0:LANES] = fa[at:at + COLS, :].astype(BF16)
        out[row, :, LANES:CH] = fb[at:at + COLS, 0:HALF].astype(BF16)

    def gates(z, bias, c_a, c_b):
        z = [z[:, lanes(n)] + bias[:, lanes(n)] for n in range(6)]
        ca_new = sigmoid(z[1]) * c_a + sigmoid(z[0]) * jnp.tanh(z[3])
        h_a = sigmoid(z[2]) * jnp.tanh(ca_new)
        out_cand = jnp.tanh(z[5] * og_in) * og_in + og_add
        turned = half_turn(out_cand)
        terms = sigmoid(z[4]) * sel(turned, c_b)
        cb_new = terms + half_turn(terms)
        h_b = sel(out_cand, turned) * jnp.tanh(cb_new)
        return h_a, h_b, ca_new, cb_new

    def unit_rows(unit):
        kind, y, count = unit
        return {"I": INNER, "E": 2 * EDGE * count, "S": 2 * STRIP}[kind]

    def unit_lhs(hb, unit):
        kind, y, count = unit
        if kind == "S":
            return sb[...]

        def block(r, part):
            if kind == "I":
                return hb[r, 0:INNER, part]
            return hb[r:r + count, INNER:COLS, part].reshape(unit_rows(unit), part.stop - part.start)

        near = [block(y + e, lanes(0, 4)) for e in range(3)]
        far = [block(y + e, lanes(4)) for e in range(3)]
        return jnp.concatenate(near + [sel(far[0], far[1]), far[2]], axis=1)

    def unit_gates(unit, z, part, bias, fa, fb):
        z = z[part, :]
        kind, y, count = unit
        if kind == "S":
            c_a, c_b = (jnp.concatenate([ext[n, 8:8 + STRIP, :] for ext in (el, er)], axis=0) for n in (5, 6))
            h_a, h_b, _, _ = gates(z, bias, c_a, c_b)
            for beside, first, there in ((-1, 0, has_left), (COLS, STRIP, has_right)):
                for ref, h in ((fa, h_a), (fb, h_b)):
                    h = jnp.where(there, h[first:first + STRIP], 0.0)
                    ref[pl.ds(at_row(1) + beside, ROWS, stride=PITCH), :] = h[0:ROWS]
                    ref[pl.ds(at_row(ROWS + 1) + beside, 1), :] = h[ROWS:ROWS + 1]
            return
        if kind == "I":
            spans = [(y, EDGE, INNER)]
        else:
            spans = [(y + n, x, EDGE) for n in range(count) for x in (0, COLS - EDGE)]
        cells = [slice(r * COLS + x, r * COLS + x + size) for r, x, size in spans]
        c_a, c_b = (jnp.concatenate([ref[part, :] for part in cells], axis=0) for ref in (ca, cb))
        h_a, h_b, ca_new, cb_new = gates(z, bias, c_a, c_b)
        done = 0
        for (r, x, size), part in zip(spans, cells):
            to = slice(at_row(r + 1) + x, at_row(r + 1) + x + size)
            for ref, where, value in ((fa, to, h_a), (fb, to, h_b), (ca, part, ca_new), (cb, part, cb_new)):
                ref[where, :] = value[done:done + size]
            done += size

    def i_units(rows):
        return [("I", y, 1) for y in rows]

    e_units = [[("E", y, 3) for y in rows[::3]] for rows in E_ROWS]
    old, new = (fa0, fb0), (fa1, fb1)
    results = [None, None]

    def piece(parity, hb, units, tasks, cut=not exchange):
        lhs = jnp.concatenate([unit_lhs(hb, unit) for unit in units], axis=0)
        if not cut:
            results[parity] = jnp.dot(lhs, w_ref[...], preferred_element_type=F32)
        else:
            half = sum(unit_rows(unit) for unit in units[:(len(units) + 1) // 2])
            wide = [jnp.dot(lhs, w_ref[:, lanes(2 * n, 2)], preferred_element_type=F32) for n in range(2)]
            halves = [jnp.dot(part, w_ref[:, lanes(4, 2)], preferred_element_type=F32) for part in (lhs[:half], lhs[half:])]
            results[parity] = jnp.concatenate(wide + [jnp.concatenate(halves, axis=0)], axis=1)
        for task in tasks:
            task()

    def gate_tasks(parity, units, bias, state):
        z = zs if parity is None else results[parity]
        tasks, first = [], 0
        for unit in units:
            size = unit_rows(unit)
            tasks.append(functools.partial(unit_gates, unit, z, slice(first, first + size), bias, *state))
            first += size
        return tasks

    def inner_tasks(state, hb, rows):
        return [functools.partial(assemble_inner, *state, hb, r) for r in rows]

    def edge_tasks(state, hb, rows):
        return [functools.partial(assemble_edge, *state, hb, r) for r in rows]

    def out_tasks(state, out, rows):
        return [functools.partial(write_out, *state, out, y) for y in rows]

    def out_copy(out, t, n):
        return cut_copy(out, refs.h_seq.at[t, 0], refs.out_sems.at[n])

    def bias_of(t):
        return bp[pl.ds(t, 1), :]

    def early(t, tasks):
        units = [i_units(rows) for rows in EARLY_ROWS]
        bias = bias_of(t)
        for n in range(4):
            more = gate_tasks(1 - n % 2, units[n - 1], bias, new) if n else []
            piece(n % 2, hb0, units[n], more + tasks[n])
        zs[...] = results[1]

    def halos(slot):
        for copy in seam_copies(slot):
            copy.wait()
        columns(slot, False)
        insert_halos(slot)

    def rest(s, slot, last):
        bias_a, bias_b = bias_of(2 * s), bias_of(2 * s + 1)
        for r in range(1, 11):
            assemble_edge(*old, hb0, r)

        far = e_units[1] + [("S", 0, 0), ("E", ROWS, 1)]
        late = i_units(LATE_ROWS)
        piece(0, hb0, e_units[0], [build_strips] + edge_tasks(old, hb0, range(11, GROWS)) + gate_tasks(None, i_units(EARLY_ROWS[3]), bias_a, new))
        piece(1, hb0, far, inner_tasks(old, hb0, range(ROWS + 1, GROWS)) + gate_tasks(0, e_units[0], bias_a, new))
        piece(0, hb0, late, gate_tasks(1, far, bias_a, new) + edge_tasks(new, hb1, range(1, 11)))

        rows = [i_units(part) for part in I_ROWS]
        piece(1, hb1, e_units[0], gate_tasks(0, late, bias_a, new) + edge_tasks(new, hb1, range(11, ROWS + 2)))
        piece(0, hb1, e_units[1], gate_tasks(1, e_units[0], bias_b, old) + inner_tasks(new, hb1, range(18, ROWS + 2)))
        piece(1, hb1, rows[3], gate_tasks(0, e_units[1], bias_b, old) + inner_tasks(new, hb1, range(1, 8)))
        if not last:
            build_messages()
            columns(1 - slot, True)
        piece(0, hb1, rows[0], gate_tasks(1, rows[3], bias_b, old) + inner_tasks(new, hb1, range(8, 18)), True)
        if not last:
            for copy in seam_copies(1 - slot):
                copy.start()
        out0, out1 = (refs.out0, refs.out1) if last else (refs.hs.at[2 * s], refs.hs.at[2 * s + 1])

        def next_operands(first, count):
            return [] if last else inner_tasks(old, hb0, range(first, first + count))

        piece(1, hb1, rows[1], gate_tasks(0, rows[0], bias_b, old) + next_operands(19, 6) + next_operands(1, 6) + out_tasks(new, out0, range(ROWS)))
        piece(0, hb1, rows[2], gate_tasks(1, rows[1], bias_b, old) + next_operands(7, 6) + out_tasks(old, out1, I_ROWS[0]) + out_tasks(old, out1, I_ROWS[3]))
        tail = gate_tasks(0, rows[2], bias_b, old) + next_operands(13, 6)
        done = out_tasks(old, out1, I_ROWS[1]) + out_tasks(old, out1, I_ROWS[2])
        if last:
            for copy in out_copy(out0, 2 * s, 0):
                copy.start()
            for task in tail + done:
                task()
            for copy in out_copy(out1, 2 * s + 1, 1):
                copy.start()
        else:
            early(2 * s + 2, [tail, done[:6], done[6:], []])

    last_pair = STEPS // 2 - 1
    hb1[0] = jnp.zeros((COLS, WIDTH), BF16)
    if exchange:
        in_copies = cut_copy(refs.h_init.at[0], refs.hin, in_sems.at[0]) + cut_copy(refs.c_init.at[0], cio, in_sems.at[1])
        for copy in in_copies:
            copy.start()
        w_copies = []
        for d in range(3):
            kd = jnp.where(core == 0, d, 2 - d)
            first = 4 * LANES * d
            pieces = [(first + LANES * dx, dx, 0, LANES) for dx in range(3)] + [(first + 3 * LANES + HALF * dx, dx, LANES, HALF) for dx in range(2)]
            for dst, dx, ch, size in pieces + [(12 * LANES + HALF * d, 2, LANES, HALF)]:
                w_copies.append(pltpu.make_async_copy(refs.w_hbm.at[kd, dx, pl.ds(ch, size)], ws_ref.at[pl.ds(dst, size)], refs.w_sems.at[len(w_copies)]))
        for copy in w_copies:
            copy.start()

        for ref in (fa0, fb0, fa1, fb1):
            ref[0:PITCH, :] = jnp.zeros((PITCH, LANES), F32)
            ref[(GROWS - 2) * PITCH:, :] = jnp.zeros((2 * PITCH, LANES), F32)
        hb0[0] = jnp.zeros((COLS, WIDTH), BF16)
        ws_ref[DEPTH - HALF:, :] = jnp.zeros((HALF, GATES), BF16)
        for ref in (el, er, from_left, from_right, diag_left, diag_right):
            ref[...] = jnp.zeros(ref.shape, F32)

        barrier = pltpu.get_barrier_semaphore()
        pl.semaphore_signal(barrier, inc=1, device_id={"rows": other}, device_id_type=MESH)
        for there, near in ((has_left, col - 1), (has_right, col + 1)):
            @pl.when(there)
            def _():
                pl.semaphore_signal(barrier, inc=1, device_id={"cols": near}, device_id_type=MESH)
                pl.semaphore_signal(barrier, inc=1, device_id={"cols": near, "rows": other}, device_id_type=MESH)

        for n, block in enumerate(gate_blocks([refs.bias_ref[:, lanes(n)] for n in range(6)])):
            bp[:, lanes(n)] = block


        for copy in in_copies:
            copy.wait()

        def load_rows(n, _):
            for k in range(4):
                y = 4 * n + k
                row = out_row(y)
                to = pl.ds(pl.multiple_of(at_row(y + 1), 8), COLS)
                cells = pl.ds(pl.multiple_of(y * COLS, COLS), COLS)
                for a, b, where, value in ((fa0, fb0, to, refs.hin[row].astype(F32)), (ca, cb, cells, cio[row])):
                    a[where, :] = value[:, 0:LANES]
                    b[where, :] = jnp.concatenate([value[:, LANES:CH]] * 2, axis=1)
            return 0

        lax.fori_loop(0, ROWS // 4, load_rows, 0)
        build_messages()

        def load_weights(n, _):
            rows = pl.ds(pl.multiple_of(n * 4 * HALF, HALF), 4 * HALF)
            blocks = gate_blocks([ws_ref[rows, lanes(i)].astype(F32) for i in range(6)])
            for i, block in enumerate(blocks):
                w_ref[rows, lanes(i)] = block.astype(BF16)
            return 0

        pl.semaphore_wait(barrier, 1 + 2 * has_left.astype(jnp.int32) + 2 * has_right.astype(jnp.int32))
        columns(0, True)
        for copy in seam_copies(0):
            copy.start()
        for copy in w_copies:
            copy.wait()
        lax.fori_loop(0, DEPTH // HALF // 4, load_weights, 0)
        for r in range(1, ROWS + 1):
            assemble_inner(*old, hb0, r)
        early(0, [[], [], [], []])

        def two_steps(s, _):
            slot = lax.rem(s, 2)
            halos(slot)
            rest(s, slot, False)
            return 0

        lax.fori_loop(0, last_pair, two_steps, 0)
        halos(last_pair % 2)
        return

    before = [pltpu.make_async_copy(refs.hs.at[t], refs.h_seq.at[t, 0], refs.step_sems.at[t]) for t in range(STEPS - 2)]
    for copy in before:
        copy.start()
    rest(last_pair, None, True)

    def store_row(y, _):
        cells = pl.ds(pl.multiple_of(y * COLS, COLS), COLS)
        row = out_row(y)
        cio[row, :, 0:LANES] = ca[cells, :]
        cio[row, :, LANES:CH] = cb[cells, 0:HALF]
        return 0

    lax.fori_loop(0, ROWS, store_row, 0)
    c_copies = cut_copy(cio, refs.c_last.at[0], in_sems.at[0])
    for copy in c_copies:
        copy.start()
    for copy in before + out_copy(refs.out0, STEPS - 2, 0) + out_copy(refs.out1, STEPS - 1, 1) + c_copies:
        copy.wait()


def solution(mesh):
    def device_fn(h_init, c_init, w_rec, gate_bias):
        hbm = pl.BlockSpec(memory_space=pltpu.HBM)
        in_vmem = pl.BlockSpec(memory_space=pltpu.VMEM)
        vmem = pltpu.VMEM
        dma = pltpu.SemaphoreType.DMA
        tile = (ROWS, COLS, CH)
        edge = (5, ROWS, LANES)
        operands = vmem((GROWS, COLS, WIDTH), BF16)
        strips = vmem((2 * STRIP, DEPTH), BF16)
        state = dict(
            hs=vmem((STEPS - 2, *tile), BF16),
            w_ref=vmem((DEPTH, GATES), BF16),
            bp=vmem((STEPS, GATES), F32),
            **{name: vmem((GROWS * PITCH, LANES), F32) for name in ("fa0", "fb0", "fa1", "fb1")},
            hb0=operands,
            **{name: vmem(((ROWS + 1) * COLS, LANES), F32) for name in ("ca", "cb")},
            zs=vmem((len(EARLY_ROWS[3]) * INNER, GATES), F32),
            **{name: vmem((7, EXT, LANES), F32) for name in ("el", "er")},
        )
        held = pl.pallas_call(
            exchange_kernel,
            out_shape=tuple(state[name] for name in STATE),
            in_specs=[hbm, hbm, hbm, in_vmem],
            out_specs=(in_vmem,) * len(STATE),
            scratch_shapes=[
                vmem((DEPTH, GATES), BF16),
                vmem(tile, BF16),
                vmem(tile, F32),
                operands,
                strips,
                *[vmem(edge, F32)] * 2,
                *[vmem((2, *edge), F32)] * 2,
                *[vmem((2, 5, 8, LANES), F32)] * 2,
                vmem((2, 6, COLS, LANES), F32),
                dma((18,)),
                dma((2, CUTS)),
                dma((4,)),
                *[dma((2,))] * 4,
                dma((6,)),
                dma((2, 6)),
            ],
            compiler_params=pltpu.CompilerParams(collective_id=0, has_side_effects=True, vmem_limit_bytes=41 * 1024 * 1024),
        )(h_init, c_init, w_rec, gate_bias)
        outs = pl.pallas_call(
            final_kernel,
            out_shape=(
                jax.ShapeDtypeStruct((STEPS, 1, *tile), BF16),
                jax.ShapeDtypeStruct((1, *tile), F32),
                *[state[name] for name in CHANGED],
            ),
            in_specs=[in_vmem] * len(STATE),
            out_specs=(hbm, hbm, *[in_vmem] * len(CHANGED)),
            input_output_aliases={STATE.index(name): 2 + n for n, name in enumerate(CHANGED)},
            scratch_shapes=[operands, strips, vmem(tile, BF16), vmem(tile, BF16), vmem(tile, F32), dma((STEPS - 2,)), dma((2, CUTS)), dma((1, CUTS))],
            compiler_params=pltpu.CompilerParams(vmem_limit_bytes=16 * 1024 * 1024),
        )(*held)
        return outs[0], outs[1]

    state_spec = P("dp", "rows", "cols", None)
    return jax.shard_map(device_fn, mesh=mesh, in_specs=(state_spec, state_spec, P(), P()), out_specs=(P(None, "dp", "rows", "cols", None), state_spec), check_vma=False)
```
